32 devices in a mesh: dp: 2 (over x), col: 4 (over z), row: 4 (over y, core).
Axes of the slice: x: 2, y: 2, z: 4, core: 2. Of those that a mesh axis runs over, the one named last changes fastest.
Arguments:
- x_norm: bfloat16 [1024, 4096], P(('dp', 'row'), 'col'), parts along dimension 0
- grad_y: bfloat16 [1024, 4096], P(('dp', 'row'), 'col'), parts along dimension 0
- w_gate: bfloat16 [4096, 10240], P('row', 'col')
- w_up: bfloat16 [4096, 10240], P('row', 'col')
- w_out: bfloat16 [10240, 4096], P('row', 'col')
Outputs:
- output 1: bfloat16 [1024, 4096], P(('dp', 'row'), 'col'), parts along dimension 0
- output 2: float32 [8192, 10240], P(('dp', 'row'), 'col'), parts along dimension 0
- output 3: float32 [8192, 10240], P(('dp', 'row'), 'col'), parts along dimension 0
- output 4: float32 [20480, 4096], P(('dp', 'row'), 'col'), parts along dimension 0
There are 2 independent parts. The reference program is written for one: setup_inputs(seed, part) draws one part's arguments, and reference() takes and returns one part's arrays. A program takes and returns all parts, laid end to end along the dimension named above; an argument that names none is the same for every part.
All inputs are finite; a program needn't handle non-finite values.
Results may differ from the reference program's by a relative error of at most 0.011032.
Values are sent between devices in bfloat16 or wider.
A program may use at most 1 GiB of HBM per device.

```python
import math
import jax
import jax.numpy as jnp
from jax import lax

D_MODEL = 4096
D_FF = 10240
TOKENS = 512
ROW_BLOCK = min(TOKENS, 1024)
BLOCK_COUNT = TOKENS // ROW_BLOCK
GELU_SCALE = math.sqrt(2.0 / math.pi)


def gelu_pair(pre_act):
    pre_f32 = pre_act.astype(jnp.float32)
    inner_arg = GELU_SCALE * (pre_f32 + 0.044715 * pre_f32 * pre_f32 * pre_f32)
    tanh_val = jnp.tanh(inner_arg)
    gelu_val = 0.5 * pre_f32 * (1.0 + tanh_val)
    gelu_der = 0.5 * (1.0 + tanh_val) + 0.5 * pre_f32 * (1.0 - tanh_val * tanh_val) * GELU_SCALE * (1.0 + 3.0 * 0.044715 * pre_f32 * pre_f32)
    return gelu_val, gelu_der


def setup_inputs(seed: int = 0, part: int = 0) -> dict:
    key_list = jax.random.split(jax.random.key(seed), 4)
    part_key = jax.random.fold_in(key_list[0], part)
    key_x, key_gy = jax.random.split(part_key, 2)
    x_norm = jax.random.normal(key_x, (TOKENS, D_MODEL), jnp.float32).astype(jnp.bfloat16)
    grad_y = jax.random.normal(key_gy, (TOKENS, D_MODEL), jnp.float32).astype(jnp.bfloat16)
    w_gate = (jax.random.normal(key_list[1], (D_MODEL, D_FF), jnp.float32) * D_MODEL ** -0.5).astype(jnp.bfloat16)
    w_up = (jax.random.normal(key_list[2], (D_MODEL, D_FF), jnp.float32) * D_MODEL ** -0.5).astype(jnp.bfloat16)
    w_out = (jax.random.normal(key_list[3], (D_FF, D_MODEL), jnp.float32) * D_FF ** -0.5).astype(jnp.bfloat16)
    return {"x_norm": x_norm, "grad_y": grad_y, "w_gate": w_gate, "w_up": w_up, "w_out": w_out}


def reference(x_norm, grad_y, w_gate, w_up, w_out):
    x_blocks = x_norm.reshape(BLOCK_COUNT, ROW_BLOCK, D_MODEL)
    gy_blocks = grad_y.reshape(BLOCK_COUNT, ROW_BLOCK, D_MODEL)

    def block_step(acc_state, blk_pair):
        acc_gate, acc_up, acc_out = acc_state
        x_blk, gy_blk = blk_pair
        pre_gate = jnp.dot(x_blk, w_gate, preferred_element_type=jnp.float32).astype(jnp.bfloat16)
        pre_up = jnp.dot(x_blk, w_up, preferred_element_type=jnp.float32).astype(jnp.bfloat16)
        gelu_val, gelu_der = gelu_pair(pre_gate)
        up_f32 = pre_up.astype(jnp.float32)
        hidden = (gelu_val * up_f32).astype(jnp.bfloat16)
        grad_h = jnp.dot(gy_blk, w_out.T, preferred_element_type=jnp.float32)
        grad_gate = (grad_h * up_f32 * gelu_der).astype(jnp.bfloat16)
        grad_up = (grad_h * gelu_val).astype(jnp.bfloat16)
        grad_x = (jnp.dot(grad_gate, w_gate.T, preferred_element_type=jnp.float32) + jnp.dot(grad_up, w_up.T, preferred_element_type=jnp.float32)).astype(jnp.bfloat16)
        acc_gate = acc_gate + jnp.dot(x_blk.T, grad_gate, preferred_element_type=jnp.float32)
        acc_up = acc_up + jnp.dot(x_blk.T, grad_up, preferred_element_type=jnp.float32)
        acc_out = acc_out + jnp.dot(hidden.T, gy_blk, preferred_element_type=jnp.float32)
        return (acc_gate, acc_up, acc_out), grad_x

    zero_state = (jnp.zeros((D_MODEL, D_FF), jnp.float32), jnp.zeros((D_MODEL, D_FF), jnp.float32), jnp.zeros((D_FF, D_MODEL), jnp.float32))
    grads, gx_blocks = lax.scan(block_step, zero_state, (x_blocks, gy_blocks))
    dw_gate, dw_up, dw_out = grads
    return gx_blocks.reshape(TOKENS, D_MODEL), dw_gate, dw_up, dw_out
```

```python
import math
import jax
import jax.numpy as jnp
from jax import lax
from jax.sharding import PartitionSpec as P

GELU_SCALE = math.sqrt(2.0 / math.pi)
ROW_DIMS = (((1,), (1,)), ((), ()))
COL_DIMS = (((0,), (0,)), ((), ()))


def gelu_pair(pre_act):
    pre_f32 = pre_act.astype(jnp.float32)
    inner_arg = GELU_SCALE * (pre_f32 + 0.044715 * pre_f32 * pre_f32 * pre_f32)
    tanh_val = jnp.tanh(inner_arg)
    gelu_val = 0.5 * pre_f32 * (1.0 + tanh_val)
    gelu_der = 0.5 * (1.0 + tanh_val) + 0.5 * pre_f32 * (1.0 - tanh_val * tanh_val) * GELU_SCALE * (1.0 + 3.0 * 0.044715 * pre_f32 * pre_f32)
    return gelu_val, gelu_der


def solution(mesh):
    act_spec = P(("dp", "row"), "col")
    weight_spec = P("row", "col")
    n = mesh.shape["row"]
    swap = [(c * n + r, r * n + c) for c in range(n) for r in range(n)]

    def transpose_blocks(v):
        return lax.ppermute(v, ("col", "row"), swap)

    def block_backward(x_blk, gy_blk, gate_blk, up_blk, out_blk):
        x_all = lax.all_gather(transpose_blocks(x_blk), "col", axis=0, tiled=True)
        gy_all = lax.all_gather(gy_blk, "row", axis=0, tiled=True)
        gate_part = jnp.dot(x_all, gate_blk, preferred_element_type=jnp.float32)
        up_part = jnp.dot(x_all, up_blk, preferred_element_type=jnp.float32)
        pre_gate = lax.psum_scatter(gate_part, "row", scatter_dimension=0, tiled=True).astype(jnp.bfloat16)
        pre_up = lax.psum_scatter(up_part, "row", scatter_dimension=0, tiled=True).astype(jnp.bfloat16)
        grad_h_part = lax.dot_general(gy_all, out_blk, ROW_DIMS, preferred_element_type=jnp.float32)
        grad_h = lax.psum_scatter(grad_h_part, "col", scatter_dimension=0, tiled=True)
        pre_gate = transpose_blocks(pre_gate)
        pre_up = transpose_blocks(pre_up)
        gelu_val, gelu_der = gelu_pair(pre_gate)
        up_f32 = pre_up.astype(jnp.float32)
        hidden = (gelu_val * up_f32).astype(jnp.bfloat16)
        hidden_all = lax.all_gather(hidden, "col", axis=0, tiled=True)
        grad_gate = transpose_blocks((grad_h * up_f32 * gelu_der).astype(jnp.bfloat16))
        grad_up = transpose_blocks((grad_h * gelu_val).astype(jnp.bfloat16))
        grad_gate = lax.all_gather(grad_gate, "row", axis=0, tiled=True)
        grad_up = lax.all_gather(grad_up, "row", axis=0, tiled=True)
        grad_x_part = lax.dot_general(grad_gate, gate_blk, ROW_DIMS, preferred_element_type=jnp.float32) + lax.dot_general(grad_up, up_blk, ROW_DIMS, preferred_element_type=jnp.float32)
        grad_x = transpose_blocks(lax.psum_scatter(grad_x_part, "col", scatter_dimension=0, tiled=True).astype(jnp.bfloat16))
        dw_gate = lax.dot_general(x_all, grad_gate, COL_DIMS, preferred_element_type=jnp.float32)
        dw_up = lax.dot_general(x_all, grad_up, COL_DIMS, preferred_element_type=jnp.float32)
        dw_out = lax.dot_general(hidden_all, gy_all, COL_DIMS, preferred_element_type=jnp.float32)
        return grad_x, dw_gate, dw_up, dw_out

    return jax.shard_map(block_backward, mesh=mesh, in_specs=(act_spec, act_spec, weight_spec, weight_spec, weight_spec), out_specs=(act_spec, act_spec, act_spec, act_spec), check_vma=False)
```

```python
import math
import jax
import jax.numpy as jnp
from jax import lax
from jax.experimental import pallas as pl
from jax.experimental.pallas import tpu as pltpu
from jax.sharding import PartitionSpec as P

GELU_SCALE = math.sqrt(2.0 / math.pi)
F32, BF16 = jnp.float32, jnp.bfloat16
MESH = pl.DeviceIdType.MESH
ANY = pl.BlockSpec(memory_space=pl.ANY)
NT_DIMS = (((1,), (1,)), ((), ()))
TN_DIMS = (((0,), (0,)), ((), ()))
NCH = 4
N_CUT = ((0, 256), (256, 384))


def gelu_pair(pre_f32):
    inner_arg = GELU_SCALE * (pre_f32 + 0.044715 * pre_f32 * pre_f32 * pre_f32)
    tanh_val = jnp.tanh(inner_arg)
    gelu_val = 0.5 * pre_f32 * (1.0 + tanh_val)
    gelu_der = 0.5 * (1.0 + tanh_val) + 0.5 * pre_f32 * (1.0 - tanh_val * tanh_val) * GELU_SCALE * (1.0 + 3.0 * 0.044715 * pre_f32 * pre_f32)
    return gelu_val, gelu_der


class Slots:
    def __init__(self, ref, size):
        self.ref, self.size, self.names = ref, size, {}

    def __call__(self, *name):
        i = self.names.setdefault(name, len(self.names))
        assert i < self.size
        return self.ref.at[i]


N_SEND, N_RECV, N_LOCAL = 120, 120, 40


def comm_kernel(rows, dm, ff,
                x_hbm, gy_hbm, wg_hbm, wu_hbm, wo_hbm,
                xo, dyo, dbo, ho, dxo,
                XG, DY, WV, WP, WO, AS, AR, AO, DS, DR, DO, DB, HL, HP, DXS, DXA, DXB, DXF, DXR,
                send_ref, recv_ref, local_ref):
    fq = ff // 4
    cm = dm
    rb = rows // NCH
    tc = 4 * rb
    S, R, L = Slots(send_ref, N_SEND), Slots(recv_ref, N_RECV), Slots(local_ref, N_LOCAL)
    p, z, r = lax.axis_index("dp"), lax.axis_index("col"), lax.axis_index("row")
    y, k = r // 2, r % 2
    pr, c = z // 2, z % 2
    zm, zt = z + 1 - 2 * c, z + 2 - 4 * pr
    home = y == pr
    away = y != pr
    role = jnp.where(home, 0, 1)
    zeta = jnp.where(y == 0, z, 3 - z)
    zf, zb = z + 1 - 2 * y, z - 1 + 2 * y
    jA, jB = y, 1 - y
    ro, rp = 2 * (1 - y) + k, 2 * y + 1 - k

    def dev(z_=z, r_=r, p_=p):
        return {"dp": p_, "col": z_, "row": r_}

    pending = []

    def remote(src, dst, name, to):
        return pltpu.make_async_remote_copy(src_ref=src, dst_ref=dst, send_sem=S(*name), recv_sem=R(*name), device_id=to, device_id_type=MESH)

    def send(src, dst, name, to, cond=None, last=None):
        cp = remote(src, dst, name, to)
        if cond is None:
            cp.start()
        else:
            pl.when(cond)(cp.start)
        if last is not False:
            pending.append((cond if last is None else last, cp))
        return cp

    def got(dst, name, cond=None):
        cp = remote(dst, dst, name, dev(p_=1 - p))
        if cond is None:
            cp.wait_recv()
        else:
            pl.when(cond)(cp.wait_recv)

    def local(src, dst, *name):
        return pltpu.make_async_copy(src, dst, L(*name))

    barrier = pltpu.get_barrier_semaphore()
    peers = [dev(r_=rp), dev(r_=ro), dev(r_=2 * (1 - y) + 1 - k), dev(p_=1 - p), dev(z_=zt), dev(z_=zt + 1 - 2 * (zt % 2))]
    peers += [dev(z_=zm, r_=q) for q in range(4)]
    for peer in peers:
        pl.semaphore_signal(barrier, inc=1, device_id=peer, device_id_type=MESH)
    lx = local(x_hbm, XG.at[c, :, k, y], "x")
    pl.when(home)(lx.start)
    ldy = local(gy_hbm, DY.at[c, :, k, y], "dy")
    ldy.start()
    lw = []
    for m, w in enumerate((wg_hbm, wu_hbm)):
        for q in range(4):
            cp = local(w.at[:, pl.ds(q * fq, fq)], WV.at[m, q], "w", m, q)
            cp.start()
            lw.append(cp)

    def wo_cut(q, n, cols):
        off, ln = N_CUT[n]
        return wo_hbm.at[pl.ds(pl.multiple_of(q * fq + off, 128), ln), cols]

    def wo_slot(ro_, n, j, cols):
        off, ln = N_CUT[n]
        start, width = cols
        return WO.at[ro_, pl.ds(off, ln), pl.ds(pl.multiple_of(j * cm + start, 512), width)]

    half = cm // 2
    pcols = pl.ds(pl.multiple_of(p * half, 512), half)

    lwo = []
    for n in range(2):
        cp = local(wo_cut(r, n, pl.ds(0, cm)), wo_slot(role, n, c, (0, cm)), "wo", n)
        pl.when(k == c)(cp.start)
        lwo.append(cp)
    pl.semaphore_wait(barrier, len(peers))

    send(gy_hbm, DY.at[c, :, k, y], ("dyy",), dev(r_=ro))
    for th in range(2):
        ts = pl.ds(2 * th, 2)
        send(x_hbm.at[ts], XG.at[c, ts, k, y], ("xy", th), dev(r_=ro), away)

    def wo_near(n):
        send(wo_cut(rp, n, pl.ds(0, cm)), wo_slot(role, n, c, (0, cm)), ("wo", 0, n), dev(r_=rp), k == c)
        for k2 in range(2):
            q = 2 * (1 - y) + k2
            send(wo_cut(q, n, pcols), wo_slot(role, n, c, (p * half, half)), ("wo", 1, n, k2), dev(r_=q), k == c)

    def wo_far(n, cond):
        for dy_ in (1, 0):
            for k2 in range(2):
                q = 2 * (1 - y if dy_ else y) + k2
                send(wo_cut(q, n, pcols), wo_slot(role, n, c, (p * half, half)), ("wo", 2 + dy_, n, k2), dev(z_=zm, r_=q), cond, False)

    def wo_far_pending(n):
        for dy_ in (1, 0):
            for k2 in range(2):
                q = 2 * (1 - y if dy_ else y) + k2
                pending.append((k != c, remote(wo_cut(q, n, pcols), wo_slot(role, n, c, (p * half, half)), ("wo", 2 + dy_, n, k2), dev(z_=zm, r_=q))))

    far_away, far_home = jnp.logical_and(k != c, away), jnp.logical_and(k != c, home)
    for n in range(2):
        wo_near(n)
        wo_far_pending(n)
    wo_far(0, far_away)
    for m, w in enumerate((wg_hbm, wu_hbm)):
        for s in range(2):
            send(w.at[:, pl.ds(pl.multiple_of((1 - k + 2 * s) * fq, 128), fq)], WP.at[m, s], ("w", m, s), dev(r_=rp))

    def chain_start(name, A, B):
        send(A, A, (*name, "A"), dev(z_=zf), zeta == 0, zeta <= 2)
        send(B, B, (*name, "B"), dev(z_=zf), zeta == 1, jnp.logical_or(zeta == 1, zeta == 2))
        send(B, B, (*name, "b"), dev(z_=zb), zeta == 1)

    def chain_B(name, B):
        got(B, (*name, "b"), zeta == 0)
        got(B, (*name, "B"), zeta >= 2)
        send(B, B, (*name, "B"), dev(z_=zf), zeta == 2, False)

    def chain_A(name, A):
        got(A, (*name, "A"), zeta >= 1)
        send(A, A, (*name, "A"), dev(z_=zf), jnp.logical_or(zeta == 1, zeta == 2), False)

    ldy.wait()
    got(DY.at[c, :, k, 1 - y], ("dyy",))
    send(DY.at[c, :, k], DY.at[c, :, k], ("dyz",), dev(z_=zm))
    pl.when(home)(lx.wait)
    for th in range(2):
        ts = pl.ds(2 * th, 2)
        got(XG.at[c, ts, k, 1 - y], ("xy", th), home)
        chain_start(("x", th), XG.at[jA, ts, k], XG.at[jB, ts, k])
    send(DY.at[c, :, k], DY.at[c, :, k], ("dyd", 0), dev(r_=rp))
    wo_far(0, far_home)
    wo_far(1, far_home)

    def wo_pass(a, n):
        ro_ = jnp.where(role == 0, a % 2, 1 - a % 2)
        j = c if a == 1 else 1 - c
        mine = wo_slot(ro_, n, j, (p * half, half))
        got(mine, ("wo", a, n, 0), k == 0)
        got(mine, ("wo", a, n, 1), k == 1)
        send(mine, mine, ("wx", a, n), dev(p_=1 - p))

    def wo_have(a, n):
        ro_ = jnp.where(role == 0, a % 2, 1 - a % 2)
        j = c if a < 2 else 1 - c
        if a == 0:
            pl.when(k == c)(lwo[n].wait)
            got(wo_slot(ro_, n, j, (0, cm)), ("wo", 0, n), k != c)
        else:
            got(wo_slot(ro_, n, j, ((1 - p) * half, half)), ("wx", a, n))

    for th in range(2):
        ts = pl.ds(2 * th, 2)
        chain_B(("x", th), XG.at[jB, ts, k])
        send(XG.at[jB, ts, k], XG.at[jB, ts, k], ("xd", th, "B"), dev(r_=rp))
        wo_pass(1, th)
        wo_pass(2, th)
        chain_A(("x", th), XG.at[jA, ts, k])
        send(XG.at[jA, ts, k], XG.at[jA, ts, k], ("xd", th, "A"), dev(r_=rp))
        if th == 0:
            wo_far(1, far_away)
        wo_pass(3, th)
    got(DY.at[1 - c, :, k], ("dyz",))
    send(DY.at[1 - c, :, k], DY.at[1 - c, :, k], ("dyd", 1), dev(r_=rp))
    got(DY.at[c, :, 1 - k], ("dyd", 0))
    got(DY.at[1 - c, :, 1 - k], ("dyd", 1))

    def dh_part(ro_, n, dst):
        off, ln = N_CUT[n]
        acc = None
        for j in range(2):
            t = lax.dot_general(DY[j].reshape(NCH * tc, cm), WO[ro_, off:off + ln, j * cm:(j + 1) * cm], NT_DIMS, preferred_element_type=F32)
            acc = t if acc is None else acc + t
        dst[:, off:off + ln] = acc

    def dh_mirror(n):
        for a in range(4):
            cond = home if a % 2 else away
            pl.when(cond)(lambda a=a: wo_have(a, n))
        dh_part(1, n, DS)
        off, ln = N_CUT[n]
        send(DS.at[:, pl.ds(off, ln)], DR.at[:, pl.ds(off, ln)], ("dh", n), dev(z_=zt))

    def dh_own(n):
        for a in range(4):
            cond = away if a % 2 else home
            pl.when(cond)(lambda a=a: wo_have(a, n))
        dh_part(0, n, DO)

    def ab_part(s, t, m):
        own = jnp.dot(XG[k, t].reshape(tc, cm), WV[m, k + 2 * s], preferred_element_type=F32)
        return own + jnp.dot(XG[1 - k, t].reshape(tc, cm), WP[m, s], preferred_element_type=F32)

    def ab_mirror(t):
        for m in range(2):
            AS[t, m] = ab_part(1 - y, t, m)
        send(AS.at[t], AR.at[t], ("ab", t), dev(r_=ro))

    for cp in lw:
        cp.wait()
    for m in range(2):
        for s in range(2):
            got(WP.at[m, s], ("w", m, s))
    for th in range(2):
        ts = pl.ds(2 * th, 2)
        got(XG.at[jB, ts, 1 - k], ("xd", th, "B"))
        got(XG.at[jA, ts, 1 - k], ("xd", th, "A"))
        dh_mirror(th)
        ab_mirror(2 * th)
        ab_mirror(2 * th + 1)
    out_x = local(XG.at[k], xo, "xo")
    out_x.start()
    out_dy = local(DY.at[c], dyo, "dyo")
    out_dy.start()
    dh_own(0)
    dh_own(1)

    hs = jnp.where(home, c, 2)

    def finish(t):
        for m in range(2):
            AO[m] = ab_part(y, t, m)
        got(AR.at[t], ("ab", t))
        if t == 0:
            for n, (off, ln) in enumerate(N_CUT):
                got(DR.at[:, pl.ds(off, ln)], ("dh", n))

        def body(i, _):
            rs = pl.ds(pl.multiple_of(i * 16, 16), 16)
            rt = pl.ds(pl.multiple_of(t * tc + i * 16, 16), 16)
            a = (AO[0, rs] + AR[t, 0, rs]).astype(BF16).astype(F32)
            b = (AO[1, rs] + AR[t, 1, rs]).astype(BF16).astype(F32)
            g, gd = gelu_pair(a)
            dh = DO[rt] + DR[rt]
            HL[hs, y, t, rs] = (g * b).astype(BF16)
            DB[0, r, t, rs] = (dh * b * gd).astype(BF16)
            DB[1, r, t, rs] = (dh * g).astype(BF16)
            return 0

        lax.fori_loop(0, tc // 16, body, 0)

    def share(t):
        mine = DB.at[:, r, t]
        send(mine, mine, ("dby", t), dev(r_=ro))
        send(mine, mine, ("dbd", t), dev(r_=rp))
        send(HL.at[2, y, t], HL.at[c, y, t], ("hy", t), dev(r_=ro), away)

    def relay(t):
        theirs = DB.at[:, ro, t]
        got(theirs, ("dby", t))
        send(theirs, theirs, ("dbf", t), dev(r_=rp))
        got(HL.at[c, 1 - y, t], ("hy", t), home)
        chain_start(("h", t), HL.at[jA, :, t], HL.at[jB, :, t])

    def relay_h(t):
        chain_B(("h", t), HL.at[jB, :, t])
        chain_A(("h", t), HL.at[jA, :, t])
        send(HL.at[1 - k, :, t], HP.at[:, t], ("hd", t), dev(r_=rp))

    def dx_part(t):
        got(DB.at[:, rp, t], ("dbd", t))
        got(DB.at[:, 2 * (1 - y) + 1 - k, t], ("dbf", t))
        acc = None
        for m in range(2):
            for q in range(4):
                d = lax.dot_general(DB[m, q, t], WV[m, q], NT_DIMS, preferred_element_type=F32)
                acc = d if acc is None else acc + d
        DXS[t] = acc
        z2 = jnp.where(y == 0, 2, 1)
        send(DXS.at[t], DXA.at[t], ("dxa", t), dev(z_=z2), zeta == 3)
        send(DXS.at[t], DXA.at[t], ("dxm", t), dev(z_=r), jnp.logical_and(zeta < 2, z != r))

    def dx_mid(t):
        @pl.when(zeta == 2)
        def _():
            got(DXA.at[t], ("dxa", t))
            DXS[t] += DXA[t]
        send(DXS.at[t], DXB.at[t], ("dxb", t), dev(z_=r), zeta == 2)

    diag = z == r

    def dx_end(t):
        @pl.when(diag)
        def _():
            got(DXA.at[t], ("dxm", t))
            got(DXB.at[t], ("dxb", t))
            DXF[t] = (DXS[t] + DXA[t] + DXB[t]).astype(BF16).reshape(2, 2, rb, cm)
        for k2, y2, n in ((1 - k, y, 0), (k, 1 - y, 1), (1 - k, 1 - y, 2)):
            send(DXF.at[t, k2, y2], DXR.at[t], ("dxf", t, n), dev(r_=2 * y2 + k2), diag)

    def dx_take(t):
        @pl.when(diag)
        def _():
            DXR[t] = DXF[t, k, y]
        zk, zy = z % 2, z // 2
        got(DXR.at[t], ("dxf", t, 0), jnp.logical_and(zk != k, zy == y))
        got(DXR.at[t], ("dxf", t, 1), jnp.logical_and(zk == k, zy != y))
        got(DXR.at[t], ("dxf", t, 2), jnp.logical_and(zk != k, zy != y))

    for t in range(NCH + 3):
        if t < NCH:
            finish(t)
            share(t)
        if 0 <= t - 1 < NCH:
            relay(t - 1)
            dx_part(t - 1)
        if 0 <= t - 2 < NCH:
            dx_mid(t - 2)
            relay_h(t - 2)
        if 0 <= t - 3 < NCH:
            dx_end(t - 3)
    outs = [local(DB, dbo, "dbo"), local(HL.at[k], ho.at[:, k], "ho")]
    for cp in outs:
        cp.start()
    for t in range(NCH):
        got(HP.at[:, t], ("hd", t))
        dx_take(t)
    outs += [local(HP, ho.at[:, 1 - k], "hp"), local(DXR, dxo, "dxo")]
    for cp in outs[2:]:
        cp.start()
    for cond, cp in pending:
        if cond is None:
            cp.wait_send()
        else:
            pl.when(cond)(cp.wait_send)
    for cp in outs + [out_x, out_dy]:
        cp.wait()


def dw_kernel(x_hbm, dy_hbm, db_hbm, h_hbm, dx_hbm, dwg, dwu, dwo, dxo, X, XT, DY, DB, H, OA, OB, in_sem, out_sem):
    tok, fq = X.shape[0], DB.shape[-1]
    loads = [pltpu.make_async_copy(x_hbm, X, in_sem.at[0]), pltpu.make_async_copy(dy_hbm, DY, in_sem.at[1])]
    for m in range(2):
        for q in range(4):
            loads.append(pltpu.make_async_copy(db_hbm.at[m, q], DB.at[m, q], in_sem.at[2 + 4 * m + q]))
    for q in range(4):
        loads.append(pltpu.make_async_copy(h_hbm.at[q], H.at[q], in_sem.at[10 + q]))
    for cp in loads:
        cp.start()
    loads[0].wait()
    XT[...] = X[...].T
    outs = [None, None, None, None]
    for m, dst in ((0, dwg), (1, dwu)):
        for q in range(4):
            loads[2 + 4 * m + q].wait()
            slot = q % 2
            if outs[slot] is not None:
                outs[slot].wait()
            OA[slot] = jnp.dot(XT[...], DB[m, q], preferred_element_type=F32)
            outs[slot] = pltpu.make_async_copy(OA.at[slot], dst.at[:, pl.ds(q * fq, fq)], out_sem.at[slot])
            outs[slot].start()
    loads[1].wait()
    for q in range(4):
        loads[10 + q].wait()
        slot = q % 2
        if outs[2 + slot] is not None:
            outs[2 + slot].wait()
        OB[slot] = lax.dot_general(H[q], DY[...], TN_DIMS, preferred_element_type=F32)
        outs[2 + slot] = pltpu.make_async_copy(OB.at[slot], dwo.at[pl.ds(q * fq, fq)], out_sem.at[2 + slot])
        outs[2 + slot].start()
    for cp in outs:
        cp.wait()
    dxo[...] = dx_hbm[...]


def solution(mesh):
    act_spec = P(("dp", "row"), "col")
    weight_spec = P("row", "col")

    def block_backward(x_blk, gy_blk, gate_blk, up_blk, out_blk):
        rows, dm = x_blk.shape
        ff = gate_blk.shape[1]
        fq, rb = ff // 4, rows // NCH
        tc = 4 * rb
        tok = NCH * tc
        vm = pltpu.VMEM
        xg, dyg, dbg, hg, dxg = pl.pallas_call(
            lambda *refs: comm_kernel(rows, dm, ff, *refs),
            out_shape=[
                jax.ShapeDtypeStruct((NCH, 2, 2, rb, dm), BF16),
                jax.ShapeDtypeStruct((NCH, 2, 2, rb, dm), BF16),
                jax.ShapeDtypeStruct((2, 4, NCH, tc, fq), BF16),
                jax.ShapeDtypeStruct((2, 2, NCH, tc, fq), BF16),
                jax.ShapeDtypeStruct((NCH, rb, dm), BF16),
            ],
            in_specs=[ANY] * 5,
            out_specs=[ANY] * 5,
            scratch_shapes=[
                vm((2, NCH, 2, 2, rb, dm), BF16),
                vm((2, NCH, 2, 2, rb, dm), BF16),
                vm((2, 4, dm, fq), BF16),
                vm((2, 2, dm, fq), BF16),
                vm((2, fq, 2 * dm), BF16),
                vm((NCH, 2, tc, fq), F32),
                vm((NCH, 2, tc, fq), F32),
                vm((2, tc, fq), F32),
                vm((tok, fq), F32),
                vm((tok, fq), F32),
                vm((tok, fq), F32),
                vm((2, 4, NCH, tc, fq), BF16),
                vm((3, 2, NCH, tc, fq), BF16),
                vm((2, NCH, tc, fq), BF16),
                vm((NCH, tc, dm), F32),
                vm((NCH, tc, dm), F32),
                vm((NCH, tc, dm), F32),
                vm((NCH, 2, 2, rb, dm), BF16),
                vm((NCH, rb, dm), BF16),
                pltpu.SemaphoreType.DMA((N_SEND,)),
                pltpu.SemaphoreType.DMA((N_RECV,)),
                pltpu.SemaphoreType.DMA((N_LOCAL,)),
            ],
            compiler_params=pltpu.CompilerParams(collective_id=0, has_side_effects=True, vmem_limit_bytes=63 * 1024 * 1024),
            name="comm",
        )(x_blk.reshape(NCH, rb, dm), gy_blk.reshape(NCH, rb, dm), gate_blk, up_blk, out_blk)
        whole = pl.BlockSpec(memory_space=vm)
        dw_gate, dw_up, dw_out, grad_x = pl.pallas_call(
            dw_kernel,
            out_shape=[
                jax.ShapeDtypeStruct((dm, ff), F32),
                jax.ShapeDtypeStruct((dm, ff), F32),
                jax.ShapeDtypeStruct((ff, dm), F32),
                jax.ShapeDtypeStruct((rows, dm), BF16),
            ],
            in_specs=[ANY] * 4 + [whole],
            out_specs=[ANY] * 3 + [whole],
            scratch_shapes=[
                vm((tok, dm), BF16), vm((dm, tok), BF16), vm((tok, dm), BF16),
                vm((2, 4, tok, fq), BF16), vm((4, tok, fq), BF16),
                vm((2, dm, fq), F32), vm((2, fq, dm), F32),
                pltpu.SemaphoreType.DMA((14,)), pltpu.SemaphoreType.DMA((4,)),
            ],
            compiler_params=pltpu.CompilerParams(vmem_limit_bytes=60 * 1024 * 1024),
            name="dw",
        )(xg.reshape(tok, dm), dyg.reshape(tok, dm), dbg.reshape(2, 4, tok, fq), hg.reshape(4, tok, fq), dxg.reshape(rows, dm))
        return grad_x, dw_gate, dw_up, dw_out

    return jax.shard_map(block_backward, mesh=mesh, in_specs=(act_spec, act_spec, weight_spec, weight_spec, weight_spec), out_specs=(act_spec, act_spec, act_spec, act_spec), check_vma=False)
```

```python
import math
import jax
import jax.numpy as jnp
from jax import lax
from jax.experimental import pallas as pl
from jax.experimental.pallas import tpu as pltpu
from jax.sharding import PartitionSpec as P

GELU_SCALE = math.sqrt(2.0 / math.pi)
F32, BF16 = jnp.float32, jnp.bfloat16
MESH = pl.DeviceIdType.MESH
ANY = pl.BlockSpec(memory_space=pl.ANY)
NT_DIMS = (((1,), (1,)), ((), ()))
TN_DIMS = (((0,), (0,)), ((), ()))
RBS = (48, 32, 32, 16)
NCH = len(RBS)
OFF = tuple(sum(RBS[:t]) for t in range(NCH))
X_CUT = ((0, 80), (80, 48))
N_CUT = ((0, 128), (128, 256), (384, 256))
NS = range(len(N_CUT))
N_SEND, N_RECV, N_LOCAL = 160, 160, 48


def gelu_pair(pre_f32):
    inner_arg = GELU_SCALE * (pre_f32 + 0.044715 * pre_f32 * pre_f32 * pre_f32)
    tanh_val = jnp.tanh(inner_arg)
    gelu_val = 0.5 * pre_f32 * (1.0 + tanh_val)
    gelu_der = 0.5 * (1.0 + tanh_val) + 0.5 * pre_f32 * (1.0 - tanh_val * tanh_val) * GELU_SCALE * (1.0 + 3.0 * 0.044715 * pre_f32 * pre_f32)
    return gelu_val, gelu_der


class Slots:
    def __init__(self, ref, size):
        self.ref, self.size, self.names = ref, size, {}

    def __call__(self, *name):
        i = self.names.setdefault(name, len(self.names))
        assert i < self.size
        return self.ref.at[i]


def comm_kernel(rows, dm, ff,
                x_hbm, gy_hbm, wg_hbm, wu_hbm, wo_hbm,
                xo, dyo, dbo, ho, dxo,
                XG, XR, DY, WV, WP, WO, WR, AS, AR, AO, DS, DR, DO, DB, HL, HP, DXS, DXA, DXM, DXF, DXR, XT,
                send_ref, recv_ref, local_ref):
    fq = ff // 4
    cm = dm
    S, R, L = Slots(send_ref, N_SEND), Slots(recv_ref, N_RECV), Slots(local_ref, N_LOCAL)
    p, z, r = lax.axis_index("dp"), lax.axis_index("col"), lax.axis_index("row")
    y, k = r // 2, r % 2
    pr, c = z // 2, z % 2
    zm, zt = z + 1 - 2 * c, z + 2 - 4 * pr
    home, away = y == pr, y != pr
    role = jnp.where(home, 0, 1)
    zeta = jnp.where(y == 0, z, 3 - z)
    zf, zb = z + 1 - 2 * y, z - 1 + 2 * y
    z2 = jnp.where(y == 0, 2, 1)
    jA, jB = y, 1 - y
    ro, rp = 2 * (1 - y) + k, 2 * y + 1 - k
    rx = 2 * (1 - y) + 1 - k
    diag = z == r

    def both(a, b):
        return jnp.logical_and(a, b)

    def dev(z_=z, r_=r, p_=p):
        return {"dp": p_, "col": z_, "row": r_}

    pending = []

    def remote(src, dst, name, to):
        return pltpu.make_async_remote_copy(src_ref=src, dst_ref=dst, send_sem=S(*name), recv_sem=R(*name), device_id=to, device_id_type=MESH)

    def send(src, dst, name, to, cond=None, last=None):
        cp = remote(src, dst, name, to)
        if cond is None:
            cp.start()
        else:
            pl.when(cond)(cp.start)
        if last is not False:
            pending.append((cond if last is None else None if last is True else last, cp))

    def got(dst, name, cond=None):
        cp = remote(dst, dst, name, dev(p_=1 - p))
        if cond is None:
            cp.wait_recv()
        else:
            pl.when(cond)(cp.wait_recv)

    def local(src, dst, *name):
        return pltpu.make_async_copy(src, dst, L(*name))

    barrier = pltpu.get_barrier_semaphore()
    peers = [dev(r_=rp), dev(r_=ro), dev(r_=rx), dev(p_=1 - p), dev(z_=zt), dev(z_=zt + 1 - 2 * (zt % 2))]
    peers += [dev(z_=zm, r_=q) for q in range(4)]
    for peer in peers:
        pl.semaphore_signal(barrier, inc=1, device_id=peer, device_id_type=MESH)

    @pl.when(jnp.logical_not(diag))
    def _():
        pl.semaphore_signal(barrier, inc=1, device_id=dev(z_=r, r_=z), device_id_type=MESH)

    lx = local(x_hbm, XG.at[c, k, y], "x")
    pl.when(home)(lx.start)
    ldy = local(gy_hbm, DY.at[c, k, y], "dy")
    ldy.start()
    lw = []
    for m, w in enumerate((wg_hbm, wu_hbm)):
        for q in range(4):
            cp = local(w.at[:, pl.ds(q * fq, fq)], WV.at[q, :, pl.ds(m * fq, fq)], "w", m, q)
            cp.start()
            lw.append(cp)

    def wo_cut(q, n, cols):
        off, ln = N_CUT[n]
        return wo_hbm.at[pl.ds(pl.multiple_of(q * fq + off, 128), ln), cols]

    def wo_slot(ro_, n, j, cols):
        off, ln = N_CUT[n]
        start, width = cols
        return WO.at[ro_, pl.ds(off, ln), pl.ds(pl.multiple_of(j * cm + start, 512), width)]

    half = cm // 2
    pcols = pl.ds(pl.multiple_of(p * half, 512), half)
    lwo = []
    for n in NS:
        cp = local(wo_cut(r, n, pl.ds(0, cm)), wo_slot(role, n, c, (0, cm)), "wo", n)
        pl.when(k == c)(cp.start)
        lwo.append(cp)
    pl.semaphore_wait(barrier, jnp.where(diag, len(peers), len(peers) + 1))

    def chunk(t):
        return pl.ds(OFF[t], RBS[t])

    def x_place(src_z, ts, cond):
        mine = src_z // 2 == y
        return ((XG.at[src_z % 2, k, y, ts], both(cond, mine)), (XR.at[src_z % 2, ts], both(cond, jnp.logical_not(mine))))

    def x_send(th):
        ts = pl.ds(*X_CUT[th])
        for name, to, cond in (("xr", z + 1, z < 3), ("xl", z - 1, z > 0)):
            for dst, ok in x_place(z, ts, cond):
                send(x_hbm.at[ts], dst, (name, th, 1), dev(z_=to), ok)
        send(x_hbm.at[ts], XG.at[c, k, y, ts], ("xy", th, 0), dev(r_=ro), away)

    def x_step(th, d, left):
        ts = pl.ds(*X_CUT[th])
        src_z, to = (z + d, z - 1) if left else (z - d, z + 1)
        here = src_z <= 3 if left else src_z >= 0
        more = both(here, to >= 0 if left else to <= 3)
        name = "xl" if left else "xr"
        for ref, ok in x_place(src_z, ts, here):
            got(ref, (name, th, d), ok)
            if d < 3:
                send(ref, ref, (name, th, d + 1), dev(z_=to), both(ok, more))
        ref, ok = x_place(src_z, ts, here)[1]
        same = src_z % 2 == c
        send(ref, XG.at[src_z % 2, k, y, ts], ("xy", th, 0), dev(r_=ro), both(ok, same))
        send(ref, XG.at[src_z % 2, k, y, ts], ("xy", th, 1), dev(r_=ro), both(ok, jnp.logical_not(same)))

    def x_give(th):
        ts = pl.ds(*X_CUT[th])
        if th == 0:
            pl.when(home)(lx.wait)
        got(XG.at[c, k, 1 - y, ts], ("xy", th, 0))
        got(XG.at[1 - c, k, 1 - y, ts], ("xy", th, 1))
        send(XG.at[:, k, :, ts], XG.at[:, k, :, ts], ("xd", th), dev(r_=rp))

    def x_take(th):
        got(XG.at[:, 1 - k, :, pl.ds(*X_CUT[th])], ("xd", th))

    def dy_pass():
        ldy.wait()
        got(DY.at[c, k, 1 - y], ("dyy",))
        send(DY.at[c, k], DY.at[c, k], ("dyz",), dev(z_=zm))
        send(DY.at[c, k], DY.at[c, k], ("dyd", 0), dev(r_=rp))

    def dy_give():
        got(DY.at[1 - c, k], ("dyz",))
        send(DY.at[1 - c, k], DY.at[1 - c, k], ("dyd", 1), dev(r_=rp))

    def dy_take():
        for i, j in enumerate((c, 1 - c)):
            got(DY.at[j, 1 - k], ("dyd", i))

    def wo_near(n, cond):
        send(wo_cut(rp, n, pl.ds(0, cm)), wo_slot(role, n, c, (0, cm)), ("wo", 0, n), dev(r_=rp), both(cond, k == c))
        for k2 in range(2):
            q = 2 * (1 - y) + k2
            send(wo_cut(q, n, pcols), wo_slot(role, n, c, (p * half, half)), ("wo", 1, n, k2), dev(r_=q), both(cond, k == c))

    def wo_far(n, cond):
        off, ln = N_CUT[n]
        for over in (0, 1):
            for k2 in range(2):
                q = 2 * (1 - y if over else y) + k2
                dst = WR.at[pl.ds(off, ln)] if over else wo_slot(role, n, c, (p * half, half))
                send(wo_cut(q, n, pcols), dst, ("wf" if over else "wo", 2, n, k2), dev(z_=zm, r_=2 * y + k2), both(cond, k != c))

    def wo_relay(n, cond):
        off, ln = N_CUT[n]
        for k2 in range(2):
            got(WR.at[pl.ds(off, ln)], ("wf", 2, n, k2), both(cond, k == k2))
        send(WR.at[pl.ds(off, ln)], wo_slot(role, n, 1 - c, (p * half, half)), ("wo", 3, n), dev(r_=ro), cond)

    def wo_role(a):
        return jnp.where(home, a % 2, 1 - a % 2)

    def wo_pass(a, n, cond):
        j = c if a == 1 else 1 - c
        mine = wo_slot(wo_role(a), n, j, (p * half, half))
        if a == 3:
            got(mine, ("wo", a, n), cond)
        else:
            for k2 in range(2):
                got(mine, ("wo", a, n, k2), both(cond, k == k2))
        send(mine, mine, ("wx", a, n), dev(p_=1 - p), cond)

    def wo_have(a, n, cond):
        j = c if a < 2 else 1 - c
        if a == 0:
            pl.when(both(cond, k == c))(lwo[n].wait)
            got(wo_slot(wo_role(a), n, j, (0, cm)), ("wo", 0, n), both(cond, k != c))
        else:
            got(wo_slot(wo_role(a), n, j, ((1 - p) * half, half)), ("wx", a, n), cond)

    def dh_part(ro_, n, dst):
        off, ln = N_CUT[n]
        acc = None
        for j in range(2):
            t = lax.dot_general(DY[j].reshape(4 * rows, cm), WO[ro_, off:off + ln, j * cm:(j + 1) * cm], NT_DIMS, preferred_element_type=F32)
            acc = t if acc is None else acc + t
        dst[:, :, off:off + ln] = acc.reshape(4, rows, ln)

    def dh_cols(n, t):
        off, ln = N_CUT[n]
        return slice(None), chunk(t) if n == NS[-1] else pl.ds(0, rows), pl.ds(off, ln)

    def dh_mirror(n):
        for a in range(4):
            wo_have(a, n, home if a % 2 else away)
        dh_part(1, n, DS)
        for t in range(NCH if n == NS[-1] else 1):
            send(DS.at[dh_cols(n, t)], DR.at[dh_cols(n, t)], ("dh", n, t), dev(z_=zt))

    def dh_own(n):
        for a in range(4):
            wo_have(a, n, away if a % 2 else home)
        dh_part(0, n, DO)

    def ab_part(s, t):
        tc = 4 * RBS[t]
        own = jnp.dot(XG[k, :, :, OFF[t]:OFF[t] + RBS[t]].reshape(tc, cm), WV[k + 2 * s], preferred_element_type=F32)
        other = jnp.dot(XG[1 - k, :, :, OFF[t]:OFF[t] + RBS[t]].reshape(tc, cm), WP[s], preferred_element_type=F32)
        return (own + other).reshape(4, RBS[t], 2 * fq)

    def ab_mirror(t, cond=None, last=True):
        def go():
            AS[:, OFF[t]:OFF[t] + RBS[t]] = ab_part(1 - y, t)

        go() if cond is None else pl.when(cond)(go)
        send(AS.at[:, chunk(t)], AR.at[:, chunk(t)], ("ab", t), dev(r_=ro), cond, last)

    def weights_here():
        for cp in lw:
            cp.wait()
        for m in range(2):
            for s in range(2):
                got(WP.at[s, :, pl.ds(m * fq, fq)], ("w", m, s))

    hs = jnp.where(home, c, 2)

    def row_blocks(t, fn):
        nb = RBS[t] // 16

        def body(i, _):
            fn(i // nb, pl.ds(pl.multiple_of(OFF[t] + i % nb * 16, 16), 16))
            return 0

        lax.fori_loop(0, 4 * nb, body, 0)

    def finish_ab(t):
        def own():
            AO[:, :RBS[t]] = ab_part(y, t)

        own()
        got(AR.at[:, chunk(t)], ("ab", t))

        def body(o, rs):
            ra = pl.ds(pl.multiple_of(rs.start - OFF[t], 16), 16)
            a = (AO[o, ra, :fq] + AR[o, rs, :fq]).astype(BF16).astype(F32)
            b = (AO[o, ra, fq:] + AR[o, rs, fq:]).astype(BF16).astype(F32)
            g, gd = gelu_pair(a)
            HL[hs, y, o, rs] = (g * b).astype(BF16)
            AR[o, rs, :fq] = b * gd
            AR[o, rs, fq:] = g

        row_blocks(t, body)
        send(HL.at[2, y, :, chunk(t)], HL.at[c, y, :, chunk(t)], ("hy", t), dev(r_=ro), away)

    def finish_dh(t):
        for n in NS:
            if n == NS[-1] or t == 0:
                got(DR.at[dh_cols(n, t)], ("dh", n, t))

        def body(o, rs):
            dh = DO[o, rs] + DR[o, rs]
            DB[r, o, rs, :fq] = (dh * AR[o, rs, :fq]).astype(BF16)
            DB[r, o, rs, fq:] = (dh * AR[o, rs, fq:]).astype(BF16)

        row_blocks(t, body)
        mine = DB.at[r, :, chunk(t)]
        send(mine, mine, ("dby", t), dev(r_=ro))
        send(mine, mine, ("dbd", t), dev(r_=rp))

    def relay_db(t):
        theirs = DB.at[ro, :, chunk(t)]
        got(theirs, ("dby", t))
        send(theirs, theirs, ("dbf", t), dev(r_=rp))

    def h_start(t):
        A, B = HL.at[jA, :, :, chunk(t)], HL.at[jB, :, :, chunk(t)]
        got(HL.at[c, 1 - y, :, chunk(t)], ("hy", t), home)
        send(A, A, ("hA", t), dev(z_=zf), zeta == 0, zeta <= 2)
        send(B, B, ("hB", t), dev(z_=zf), zeta == 1, both(zeta >= 1, zeta <= 2))
        send(B, B, ("hb", t), dev(z_=zb), zeta == 1)

    def h_pass(t, i):
        if i == 0:
            B = HL.at[jB, :, :, chunk(t)]
            got(B, ("hB", t), zeta == 2)
            send(B, B, ("hB", t), dev(z_=zf), zeta == 2, False)
        else:
            A = HL.at[jA, :, :, chunk(t)]
            got(A, ("hA", t), zeta == i)
            send(A, A, ("hA", t), dev(z_=zf), zeta == i, False)

    def h_last(t):
        A, B = HL.at[jA, :, :, chunk(t)], HL.at[jB, :, :, chunk(t)]
        got(B, ("hb", t), zeta == 0)
        got(B, ("hB", t), zeta == 3)
        got(A, ("hA", t), zeta == 3)
        send(HL.at[1 - k, :, :, chunk(t)], HP.at[:, :, chunk(t)], ("hd", t), dev(r_=rp))
        out(HL.at[k, :, :, chunk(t)], ho.at[:, k, :, chunk(t)], "ho", t)

    outs = []

    def out(src, dst, *name):
        cp = local(src, dst, *name)
        cp.start()
        outs.append(cp)

    target = jnp.where(y == 0, k, 1 - k)
    top = NCH - 1

    def dx_part(t, i):
        q = (r, rp, ro, rx)[i]
        theirs = DB.at[q, :, chunk(t)]
        if i == 1:
            got(theirs, ("dbd", t))
        if i == 3:
            got(theirs, ("dbf", t))
            out(DB.at[:, :, chunk(t)], dbo.at[:, :, chunk(t)], "dbo", t)
        sl = slice(OFF[t], OFF[t] + RBS[t])

        def go():
            d = lax.dot_general(DB[q, :, sl].reshape(4 * RBS[t], 2 * fq), WV[q], NT_DIMS, preferred_element_type=F32).reshape(2, 2, RBS[t], cm)
            DXS[:, :, sl] = d if i == 0 else DXS[:, :, sl] + d

        go()
        if i < 3:
            return
        mine = DXS.at[:, :, chunk(t)]
        if t < top:
            send(mine, DXA.at[:, :, chunk(t)], ("dxa", t), dev(z_=zb), zeta == 3, False)
            send(mine, DXM.at[:, :, chunk(t)], ("dxm", t), dev(z_=zf), both(zeta == 0, target == 1))
        else:
            send(DXS.at[1 - c, :, chunk(t)], DXA.at[0, :, chunk(t)], ("dx1",), dev(z_=zm))

    def dx_add(t, cond, parts):
        sl = slice(OFF[t], OFF[t] + RBS[t])

        def go():
            for ref in parts:
                DXS[:, :, sl] += ref[:, :, sl]

        pl.when(cond)(go)

    def dx_step(t, at):
        on = zeta == at
        goes = both(on, at > target) if at else both(on, target < 0)
        got(DXA.at[:, :, chunk(t)], ("dxa", t), both(on, at >= target))
        if at == 1:
            got(DXM.at[:, :, chunk(t)], ("dxm", t), both(on, target == 1))
            dx_add(t, both(on, target == 1), (DXA, DXM))
            dx_add(t, both(on, target == 0), (DXA,))
        else:
            dx_add(t, both(on, at >= target), (DXA,))
        if at:
            send(DXS.at[:, :, chunk(t)], DXA.at[:, :, chunk(t)], ("dxa", t), dev(z_=zb), goes, both(zeta >= 1, zeta > target) if at == 1 else False)

    def dx_spread(t):
        sl = slice(OFF[t], OFF[t] + RBS[t])

        @pl.when(diag)
        def _():
            DXF.__setitem__((slice(None), slice(None), sl), DXS[:, :, sl].astype(BF16))

        for k2, y2, i in ((1 - k, y, 0), (k, 1 - y, 1), (1 - k, 1 - y, 2)):
            send(DXF.at[k2, y2, chunk(t)], DXR.at[chunk(t)], ("dxf", t, i), dev(r_=2 * y2 + k2), diag)

    def dx_half():
        t = top
        sl = slice(OFF[t], OFF[t] + RBS[t])
        got(DXA.at[0, :, chunk(t)], ("dx1",))

        def go():
            DXS[c, :, sl] += DXA[0, :, sl]

        go()
        send(DXS.at[c, 1 - pr, chunk(t)], DXM.at[0, 0, chunk(t)], ("dx2",), dev(z_=zt))

    def dx_quarter():
        t = top
        sl = slice(OFF[t], OFF[t] + RBS[t])
        got(DXM.at[0, 0, chunk(t)], ("dx2",))

        def go():
            DXF[k, y, sl] = (DXS[c, pr, sl] + DXM[0, 0, sl]).astype(BF16)

        go()
        send(DXF.at[k, y, chunk(t)], DXR.at[chunk(t)], ("dxt",), dev(z_=r, r_=z), jnp.logical_not(diag))

    def start():
        send(gy_hbm, DY.at[c, k, y], ("dyy",), dev(r_=ro))
        x_send(0)
        for m, w in enumerate((wg_hbm, wu_hbm)):
            for s in range(2):
                send(w.at[:, pl.ds(pl.multiple_of((1 - k + 2 * s) * fq, 128), fq)], WP.at[s, :, pl.ds(m * fq, fq)], ("w", m, s), dev(r_=rp))
        wo_far(0, away)
        wo_near(0, home)
        wo_near(0, away)

    def h_take(t):
        got(HP.at[:, :, chunk(t)], ("hd", t))
        out(HP.at[:, :, chunk(t)], ho.at[:, 1 - k, :, chunk(t)], "hp", t)

    def dx_take(t):
        sl = slice(OFF[t], OFF[t] + RBS[t])
        zk, zy = z % 2, z // 2

        @pl.when(diag)
        def _():
            DXR.__setitem__(sl, DXF[k, y, sl])

        if t < top:
            got(DXR.at[chunk(t)], ("dxf", t, 0), both(zk != k, zy == y))
            got(DXR.at[chunk(t)], ("dxf", t, 1), both(zk == k, zy != y))
            got(DXR.at[chunk(t)], ("dxf", t, 2), both(zk != k, zy != y))
        else:
            got(DXR.at[chunk(t)], ("dxt",), jnp.logical_not(diag))

    def out_early():
        XT.__setitem__(Ellipsis, XG[k].reshape(4 * rows, cm).T)
        out(XT, xo, "xo")
        out(DY.at[c], dyo, "dyo")

    start()
    wo_near(2, home)
    x_step(0, 1, 0)
    x_step(0, 1, 1)
    wo_far(0, home)
    x_send(1)
    x_step(0, 2, 0)
    x_step(0, 2, 1)
    wo_far(2, home)
    wo_pass(1, 0, home)
    weights_here()
    wo_near(2, away)
    wo_near(1, home)
    wo_relay(0, home)
    x_step(1, 1, 0)
    wo_far(1, away)
    wo_near(1, away)
    x_step(0, 3, 0)
    x_step(0, 3, 1)
    wo_relay(0, away)
    x_give(0)
    wo_pass(1, 0, away)
    x_step(1, 1, 1)
    x_take(0)
    dy_pass()
    x_step(1, 2, 0)
    wo_pass(1, 1, away)
    wo_pass(2, 1, away)
    ab_mirror(0, home, True)
    wo_relay(1, away)
    wo_pass(2, 0, away)
    wo_pass(3, 0, home)
    x_step(1, 2, 1)
    wo_pass(1, 1, home)
    ab_mirror(0, away, False)
    wo_far(1, home)
    dy_give()
    wo_pass(2, 0, home)
    wo_pass(3, 0, away)
    wo_pass(1, 2, home)
    wo_far(2, away)
    wo_relay(2, home)
    wo_pass(1, 2, away)
    wo_pass(3, 1, home)
    dy_take()
    dh_mirror(0)
    dh_mirror(1)
    finish_ab(0)
    x_step(1, 3, 1)
    wo_pass(2, 2, away)
    wo_relay(2, away)
    wo_pass(2, 1, home)
    ab_mirror(1)
    x_step(1, 3, 0)
    x_give(1)
    wo_pass(3, 2, away)
    wo_relay(1, home)
    dh_own(0)
    wo_pass(3, 2, home)
    wo_pass(2, 2, home)
    dh_mirror(2)
    x_take(1)
    ab_mirror(3)
    wo_pass(3, 1, away)
    h_start(0)
    dh_own(2)
    dh_own(1)
    finish_dh(0)
    out_early()
    finish_ab(1)
    ab_mirror(2)
    dx_part(0, 0)
    h_pass(0, 1)
    finish_ab(3)
    relay_db(0)
    finish_dh(1)
    dx_part(0, 1)
    h_pass(0, 0)
    dx_part(0, 2)
    dx_part(0, 3)
    h_start(1)
    finish_ab(2)
    finish_dh(3)
    h_pass(1, 1)
    h_start(3)
    h_pass(0, 2)
    finish_dh(2)
    dx_part(1, 0)
    dx_step(0, 2)
    dx_part(1, 1)
    h_pass(3, 1)
    relay_db(1)
    h_pass(1, 0)
    h_start(2)
    dx_part(1, 2)
    dx_part(1, 3)
    dx_step(0, 1)
    h_pass(1, 2)
    h_last(0)
    relay_db(3)
    dx_part(2, 0)
    relay_db(2)
    dx_part(2, 1)
    dx_part(2, 2)
    dx_step(1, 2)
    dx_part(3, 0)
    dx_part(3, 1)
    h_pass(2, 1)
    dx_part(2, 3)
    dx_part(3, 2)
    h_pass(3, 2)
    dx_part(3, 3)
    h_last(1)
    dx_step(0, 0)
    dx_step(2, 2)
    h_take(0)
    dx_step(1, 1)
    h_pass(2, 0)
    h_pass(3, 0)
    h_take(1)
    h_last(3)
    dx_step(1, 0)
    h_take(3)
    dx_spread(1)
    dx_spread(0)
    dx_half()
    dx_step(2, 1)
    dx_step(2, 0)
    dx_spread(2)
    dx_quarter()
    h_pass(2, 2)
    dx_take(0)
    h_last(2)
    dx_take(1)
    dx_take(3)
    dx_take(2)
    h_take(2)

    out(DXR, dxo, "dxo")
    for cond, cp in pending:
        if cond is None:
            cp.wait_send()
        else:
            pl.when(cond)(cp.wait_send)
    for cp in outs:
        cp.wait()


def dw_kernel(x_hbm, dy_hbm, db_hbm, h_hbm, dx_hbm, dwg, dwu, dwo, dxo, XT, DY, DB, H, OA, OB, in_sem, out_sem):
    fq = H.shape[-1]
    loads = [pltpu.make_async_copy(x_hbm, XT, in_sem.at[0])]
    loads += [pltpu.make_async_copy(db_hbm.at[q], DB.at[q], in_sem.at[1 + q]) for q in range(4)]
    loads += [pltpu.make_async_copy(dy_hbm, DY, in_sem.at[5])]
    loads += [pltpu.make_async_copy(h_hbm.at[q], H.at[q], in_sem.at[6 + q]) for q in range(4)]
    for cp in loads:
        cp.start()
    outs = []

    def put(src, dst):
        cp = pltpu.make_async_copy(src, dst, out_sem.at[len(outs)])
        cp.start()
        outs.append(cp)

    loads[0].wait()
    for q in range(4):
        loads[1 + q].wait()
        OA[q] = jnp.dot(XT[...], DB[q], preferred_element_type=F32)
        for m, dst in enumerate((dwg, dwu)):
            put(OA.at[q, :, pl.ds(m * fq, fq)], dst.at[:, pl.ds(q * fq, fq)])
    loads[5].wait()
    for q in range(4):
        loads[6 + q].wait()
        OB[q] = lax.dot_general(H[q], DY[...], TN_DIMS, preferred_element_type=F32)
        put(OB.at[q], dwo.at[pl.ds(q * fq, fq)])
    dxo[...] = dx_hbm[...]
    for cp in outs:
        cp.wait()


def solution(mesh):
    act_spec = P(("dp", "row"), "col")
    weight_spec = P("row", "col")

    def block_backward(x_blk, gy_blk, gate_blk, up_blk, out_blk):
        rows, dm = x_blk.shape
        ff = gate_blk.shape[1]
        fq, tok = ff // 4, 4 * rows
        vm = pltpu.VMEM
        xg, dyg, dbg, hg, dxg = pl.pallas_call(
            lambda *refs: comm_kernel(rows, dm, ff, *refs),
            out_shape=[
                jax.ShapeDtypeStruct((dm, tok), BF16),
                jax.ShapeDtypeStruct((2, 2, rows, dm), BF16),
                jax.ShapeDtypeStruct((4, 4, rows, 2 * fq), BF16),
                jax.ShapeDtypeStruct((2, 2, 4, rows, fq), BF16),
                jax.ShapeDtypeStruct((rows, dm), BF16),
            ],
            in_specs=[ANY] * 5,
            out_specs=[ANY] * 5,
            scratch_shapes=[
                vm((2, 2, 2, rows, dm), BF16),
                vm((2, rows, dm), BF16),
                vm((2, 2, 2, rows, dm), BF16),
                vm((4, dm, 2 * fq), BF16),
                vm((2, dm, 2 * fq), BF16),
                vm((2, fq, 2 * dm), BF16),
                vm((fq, dm // 2), BF16),
                vm((4, rows, 2 * fq), F32),
                vm((4, rows, 2 * fq), F32),
                vm((4, max(RBS), 2 * fq), F32),
                vm((4, rows, fq), F32),
                vm((4, rows, fq), F32),
                vm((4, rows, fq), F32),
                vm((4, 4, rows, 2 * fq), BF16),
                vm((3, 2, 4, rows, fq), BF16),
                vm((2, 4, rows, fq), BF16),
                vm((2, 2, rows, dm), F32),
                vm((2, 2, rows, dm), F32),
                vm((2, 2, rows, dm), F32),
                vm((2, 2, rows, dm), BF16),
                vm((rows, dm), BF16),
                vm((dm, tok), BF16),
                pltpu.SemaphoreType.DMA((N_SEND,)),
                pltpu.SemaphoreType.DMA((N_RECV,)),
                pltpu.SemaphoreType.DMA((N_LOCAL,)),
            ],
            compiler_params=pltpu.CompilerParams(collective_id=0, has_side_effects=True, vmem_limit_bytes=63 * 1024 * 1024),
            name="comm",
        )(x_blk, gy_blk, gate_blk, up_blk, out_blk)
        whole = pl.BlockSpec(memory_space=vm)
        dw_gate, dw_up, dw_out, grad_x = pl.pallas_call(
            dw_kernel,
            out_shape=[
                jax.ShapeDtypeStruct((dm, ff), F32),
                jax.ShapeDtypeStruct((dm, ff), F32),
                jax.ShapeDtypeStruct((ff, dm), F32),
                jax.ShapeDtypeStruct((rows, dm), BF16),
            ],
            in_specs=[ANY] * 4 + [whole],
            out_specs=[ANY] * 3 + [whole],
            scratch_shapes=[
                vm((dm, tok), BF16), vm((tok, dm), BF16),
                vm((4, tok, 2 * fq), BF16), vm((4, tok, fq), BF16),
                vm((4, dm, 2 * fq), F32), vm((4, fq, dm), F32),
                pltpu.SemaphoreType.DMA((10,)), pltpu.SemaphoreType.DMA((12,)),
            ],
            compiler_params=pltpu.CompilerParams(vmem_limit_bytes=60 * 1024 * 1024),
            name="dw",
        )(xg, dyg.reshape(tok, dm), dbg.reshape(4, tok, 2 * fq), hg.reshape(4, tok, fq), dxg)
        return grad_x, dw_gate, dw_up, dw_out

    return jax.shard_map(block_backward, mesh=mesh, in_specs=(act_spec, act_spec, weight_spec, weight_spec, weight_spec), out_specs=(act_spec, act_spec, act_spec, act_spec), check_vma=False)
```

```python
import math
import jax
import jax.numpy as jnp
from jax import lax
from jax.experimental import pallas as pl
from jax.experimental.pallas import tpu as pltpu
from jax.sharding import PartitionSpec as P

GELU_SCALE = math.sqrt(2.0 / math.pi)
F32, BF16 = jnp.float32, jnp.bfloat16
MESH = pl.DeviceIdType.MESH
ANY = pl.BlockSpec(memory_space=pl.ANY)
NT_DIMS = (((1,), (1,)), ((), ()))
TN_DIMS = (((0,), (0,)), ((), ()))
RBS = (32, 32, 32, 32)
NCH = len(RBS)
CHAIN = 3
OFF = tuple(sum(RBS[:t]) for t in range(NCH))
X_CUT = ((0, 64), (64, 64))
N_CUT = ((0, 128), (128, 256), (384, 256))
NS = range(len(N_CUT))
N_SEND, N_RECV, N_LOCAL = 240, 240, 64


def gelu_pair(pre_f32):
    inner_arg = GELU_SCALE * (pre_f32 + 0.044715 * pre_f32 * pre_f32 * pre_f32)
    tanh_val = jnp.tanh(inner_arg)
    gelu_val = 0.5 * pre_f32 * (1.0 + tanh_val)
    gelu_der = 0.5 * (1.0 + tanh_val) + 0.5 * pre_f32 * (1.0 - tanh_val * tanh_val) * GELU_SCALE * (1.0 + 3.0 * 0.044715 * pre_f32 * pre_f32)
    return gelu_val, gelu_der


class Slots:
    def __init__(self, ref, size):
        self.ref, self.size, self.names = ref, size, {}

    def __call__(self, *name):
        i = self.names.setdefault(name, len(self.names))
        assert i < self.size
        return self.ref.at[i]


def comm_kernel(rows, dm, ff,
                x_hbm, gy_hbm, wg_hbm, wu_hbm, wo_hbm,
                xo, dyo, dbo, ho, dxo,
                XG, XR, DY, WV, WP, WO, WR, AS, AR, AO, DS, DR, DO, DB, HL, HP, DXS, DXA, DXM, DXF, DXR, XT,
                send_ref, recv_ref, local_ref):
    fq = ff // 4
    cm = dm
    S, R, L = Slots(send_ref, N_SEND), Slots(recv_ref, N_RECV), Slots(local_ref, N_LOCAL)
    p, z, r = lax.axis_index("dp"), lax.axis_index("col"), lax.axis_index("row")
    y, k = r // 2, r % 2
    pr, c = z // 2, z % 2
    zm, zt = z + 1 - 2 * c, z + 2 - 4 * pr
    home, away = y == pr, y != pr
    role = jnp.where(home, 0, 1)
    zeta = jnp.where(y == 0, z, 3 - z)
    zf, zb = z + 1 - 2 * y, z - 1 + 2 * y
    z2 = jnp.where(y == 0, 2, 1)
    jA, jB = y, 1 - y
    ro, rp = 2 * (1 - y) + k, 2 * y + 1 - k
    rx = 2 * (1 - y) + 1 - k
    diag = z == r

    def both(a, b):
        return jnp.logical_and(a, b)

    def dev(z_=z, r_=r, p_=p):
        return {"dp": p_, "col": z_, "row": r_}

    pending = []

    def remote(src, dst, name, to):
        return pltpu.make_async_remote_copy(src_ref=src, dst_ref=dst, send_sem=S(*name), recv_sem=R(*name), device_id=to, device_id_type=MESH)

    def send(src, dst, name, to, cond=None, last=None):
        cp = remote(src, dst, name, to)
        if cond is None:
            cp.start()
        else:
            pl.when(cond)(cp.start)
        if last is not False:
            pending.append((cond if last is None else None if last is True else last, cp))

    def got(dst, name, cond=None):
        cp = remote(dst, dst, name, dev(p_=1 - p))
        if cond is None:
            cp.wait_recv()
        else:
            pl.when(cond)(cp.wait_recv)

    def local(src, dst, *name):
        return pltpu.make_async_copy(src, dst, L(*name))

    barrier = pltpu.get_barrier_semaphore()
    peers = [dev(r_=rp), dev(r_=ro), dev(r_=rx), dev(p_=1 - p), dev(z_=zt), dev(z_=zt + 1 - 2 * (zt % 2))]
    peers += [dev(z_=zm, r_=q) for q in range(4)]
    for peer in peers:
        pl.semaphore_signal(barrier, inc=1, device_id=peer, device_id_type=MESH)

    @pl.when(jnp.logical_not(diag))
    def _():
        pl.semaphore_signal(barrier, inc=1, device_id=dev(z_=r, r_=z), device_id_type=MESH)

    lx = local(x_hbm, XG.at[c, k, y], "x")
    pl.when(home)(lx.start)
    ldy = local(gy_hbm, DY.at[c, k, y], "dy")
    ldy.start()
    lw = []
    for m, w in enumerate((wg_hbm, wu_hbm)):
        for q in range(4):
            cp = local(w.at[:, pl.ds(q * fq, fq)], WV.at[q, :, pl.ds(m * fq, fq)], "w", m, q)
            cp.start()
            lw.append(cp)

    def wo_cut(q, n, cols):
        off, ln = N_CUT[n]
        return wo_hbm.at[pl.ds(pl.multiple_of(q * fq + off, 128), ln), cols]

    def wo_slot(ro_, n, j, cols):
        off, ln = N_CUT[n]
        start, width = cols
        return WO.at[ro_, pl.ds(off, ln), pl.ds(pl.multiple_of(j * cm + start, 512), width)]

    half = cm // 2
    pcols = pl.ds(pl.multiple_of(p * half, 512), half)
    lwo = []
    for n in NS:
        cp = local(wo_cut(r, n, pl.ds(0, cm)), wo_slot(role, n, c, (0, cm)), "wo", n)
        pl.when(k == c)(cp.start)
        lwo.append(cp)
    pl.semaphore_wait(barrier, jnp.where(diag, len(peers), len(peers) + 1))

    def chunk(t):
        return pl.ds(OFF[t], RBS[t])

    def x_place(src_z, ts, cond):
        mine = src_z // 2 == y
        return ((XG.at[src_z % 2, k, y, ts], both(cond, mine)), (XR.at[src_z % 2, ts], both(cond, jnp.logical_not(mine))))

    def x_send(th):
        ts = pl.ds(*X_CUT[th])
        for name, to, cond in (("xr", z + 1, z < 3), ("xl", z - 1, z > 0)):
            for dst, ok in x_place(z, ts, cond):
                send(x_hbm.at[ts], dst, (name, th, 1), dev(z_=to), ok)
        send(x_hbm.at[ts], XG.at[c, k, y, ts], ("xy", th, 0), dev(r_=ro), away)

    def x_step(th, d, left):
        ts = pl.ds(*X_CUT[th])
        src_z, to = (z + d, z - 1) if left else (z - d, z + 1)
        here = src_z <= 3 if left else src_z >= 0
        more = both(here, to >= 0 if left else to <= 3)
        name = "xl" if left else "xr"
        for ref, ok in x_place(src_z, ts, here):
            got(ref, (name, th, d), ok)
            if d < 3:
                send(ref, ref, (name, th, d + 1), dev(z_=to), both(ok, more))
        ref, ok = x_place(src_z, ts, here)[1]
        same = src_z % 2 == c
        send(ref, XG.at[src_z % 2, k, y, ts], ("xy", th, 0), dev(r_=ro), both(ok, same))
        send(ref, XG.at[src_z % 2, k, y, ts], ("xy", th, 1), dev(r_=ro), both(ok, jnp.logical_not(same)))

    def x_give(th):
        ts = pl.ds(*X_CUT[th])
        if th == 0:
            pl.when(home)(lx.wait)
        got(XG.at[c, k, 1 - y, ts], ("xy", th, 0))
        got(XG.at[1 - c, k, 1 - y, ts], ("xy", th, 1))
        send(XG.at[:, k, :, ts], XG.at[:, k, :, ts], ("xd", th), dev(r_=rp))

    def x_take(th):
        got(XG.at[:, 1 - k, :, pl.ds(*X_CUT[th])], ("xd", th))

    def dy_pass():
        ldy.wait()
        got(DY.at[c, k, 1 - y], ("dyy",))
        send(DY.at[c, k], DY.at[c, k], ("dyz",), dev(z_=zm))
        send(DY.at[c, k], DY.at[c, k], ("dyd", 0), dev(r_=rp))

    def dy_give():
        got(DY.at[1 - c, k], ("dyz",))
        send(DY.at[1 - c, k], DY.at[1 - c, k], ("dyd", 1), dev(r_=rp))

    def dy_take():
        for i, j in enumerate((c, 1 - c)):
            got(DY.at[j, 1 - k], ("dyd", i))

    def wo_near(n, cond):
        send(wo_cut(rp, n, pl.ds(0, cm)), wo_slot(role, n, c, (0, cm)), ("wo", 0, n), dev(r_=rp), both(cond, k == c))
        for k2 in range(2):
            q = 2 * (1 - y) + k2
            send(wo_cut(q, n, pcols), wo_slot(role, n, c, (p * half, half)), ("wo", 1, n, k2), dev(r_=q), both(cond, k == c))

    def wo_far(n, over, cond):
        off, ln = N_CUT[n]
        for k2 in range(2):
            q = 2 * (1 - y if over else y) + k2
            dst = WR.at[pl.ds(off, ln)] if over else wo_slot(role, n, c, (p * half, half))
            send(wo_cut(q, n, pcols), dst, ("wf" if over else "wo", 2, n, k2), dev(z_=zm, r_=2 * y + k2), both(cond, k != c))

    def wo_relay(n, cond):
        off, ln = N_CUT[n]
        for k2 in range(2):
            got(WR.at[pl.ds(off, ln)], ("wf", 2, n, k2), both(cond, k == k2))
        send(WR.at[pl.ds(off, ln)], wo_slot(role, n, 1 - c, (p * half, half)), ("wo", 3, n), dev(r_=ro), cond)

    def wo_role(a):
        return jnp.where(home, a % 2, 1 - a % 2)

    def wo_pass(a, n, cond):
        j = c if a == 1 else 1 - c
        mine = wo_slot(wo_role(a), n, j, (p * half, half))
        if a == 3:
            got(mine, ("wo", a, n), cond)
        else:
            for k2 in range(2):
                got(mine, ("wo", a, n, k2), both(cond, k == k2))
        send(mine, mine, ("wx", a, n), dev(p_=1 - p), cond)

    def wo_have(a, n, cond):
        j = c if a < 2 else 1 - c
        if a == 0:
            pl.when(both(cond, k == c))(lwo[n].wait)
            got(wo_slot(wo_role(a), n, j, (0, cm)), ("wo", 0, n), both(cond, k != c))
        else:
            got(wo_slot(wo_role(a), n, j, ((1 - p) * half, half)), ("wx", a, n), cond)

    def dh_part(ro_, n, dst):
        off, ln = N_CUT[n]
        acc = None
        for j in range(2):
            t = lax.dot_general(DY[j].reshape(4 * rows, cm), WO[ro_, off:off + ln, j * cm:(j + 1) * cm], NT_DIMS, preferred_element_type=F32)
            acc = t if acc is None else acc + t
        dst[:, :, off:off + ln] = acc.reshape(4, rows, ln)

    def dh_cols(n, t):
        off, ln = N_CUT[n]
        return slice(None), chunk(t) if n == NS[-1] else pl.ds(0, rows), pl.ds(off, ln)

    def dh_mirror(n):
        for a in range(4):
            wo_have(a, n, home if a % 2 else away)
        dh_part(1, n, DS)
        for t in range(NCH if n == NS[-1] else 1):
            send(DS.at[dh_cols(n, t)], DR.at[dh_cols(n, t)], ("dh", n, t), dev(z_=zt))

    def dh_own(n):
        for a in range(4):
            wo_have(a, n, away if a % 2 else home)
        dh_part(0, n, DO)

    def ab_part(s, t):
        tc = 4 * RBS[t]
        own = jnp.dot(XG[k, :, :, OFF[t]:OFF[t] + RBS[t]].reshape(tc, cm), WV[k + 2 * s], preferred_element_type=F32)
        other = jnp.dot(XG[1 - k, :, :, OFF[t]:OFF[t] + RBS[t]].reshape(tc, cm), WP[s], preferred_element_type=F32)
        return (own + other).reshape(4, RBS[t], 2 * fq)

    def ab_mirror(t, cond=None, last=True):
        def go():
            AS[:, OFF[t]:OFF[t] + RBS[t]] = ab_part(1 - y, t)

        go() if cond is None else pl.when(cond)(go)
        send(AS.at[:, chunk(t)], AR.at[:, chunk(t)], ("ab", t), dev(r_=ro), cond, last)

    def weights_here():
        for cp in lw:
            cp.wait()
        for m in range(2):
            for s in range(2):
                got(WP.at[s, :, pl.ds(m * fq, fq)], ("w", m, s))

    hs = jnp.where(home, c, 2)

    def row_blocks(t, fn):
        nb = RBS[t] // 16

        def body(i, _):
            fn(i // nb, pl.ds(pl.multiple_of(OFF[t] + i % nb * 16, 16), 16))
            return 0

        lax.fori_loop(0, 4 * nb, body, 0)

    def finish_ab(t):
        def own():
            AO[:, :RBS[t]] = ab_part(y, t)

        own()
        got(AR.at[:, chunk(t)], ("ab", t))

        def body(o, rs):
            ra = pl.ds(pl.multiple_of(rs.start - OFF[t], 16), 16)
            a = (AO[o, ra, :fq] + AR[o, rs, :fq]).astype(BF16).astype(F32)
            b = (AO[o, ra, fq:] + AR[o, rs, fq:]).astype(BF16).astype(F32)
            g, gd = gelu_pair(a)
            HL[hs, y, o, rs] = (g * b).astype(BF16)
            AR[o, rs, :fq] = b * gd
            AR[o, rs, fq:] = g

        row_blocks(t, body)
        send(HL.at[2, y, :, chunk(t)], HL.at[c, y, :, chunk(t)], ("hy", t), dev(r_=ro), away)

    def finish_dh(t):
        for n in NS:
            if n == NS[-1] or t == 0:
                got(DR.at[dh_cols(n, t)], ("dh", n, t))

        def body(o, rs):
            dh = DO[o, rs] + DR[o, rs]
            DB[r, o, rs, :fq] = (dh * AR[o, rs, :fq]).astype(BF16)
            DB[r, o, rs, fq:] = (dh * AR[o, rs, fq:]).astype(BF16)

        row_blocks(t, body)
        mine = DB.at[r, :, chunk(t)]
        send(mine, mine, ("dby", t), dev(r_=ro))
        send(mine, mine, ("dbd", t), dev(r_=rp))

    def relay_db(t):
        theirs = DB.at[ro, :, chunk(t)]
        got(theirs, ("dby", t))
        send(theirs, theirs, ("dbf", t), dev(r_=rp))

    def h_start(t):
        A, B = HL.at[jA, :, :, chunk(t)], HL.at[jB, :, :, chunk(t)]
        got(HL.at[c, 1 - y, :, chunk(t)], ("hy", t), home)
        send(A, A, ("hA", t), dev(z_=zf), zeta == 0, zeta <= 2)
        send(B, B, ("hB", t), dev(z_=zf), zeta == 1, both(zeta >= 1, zeta <= 2))
        send(B, B, ("hb", t), dev(z_=zb), zeta == 1)

    def h_pass(t, i):
        if i == 0:
            B = HL.at[jB, :, :, chunk(t)]
            got(B, ("hB", t), zeta == 2)
            send(B, B, ("hB", t), dev(z_=zf), zeta == 2, False)
        else:
            A = HL.at[jA, :, :, chunk(t)]
            got(A, ("hA", t), zeta == i)
            send(A, A, ("hA", t), dev(z_=zf), zeta == i, False)

    def h_last(t):
        A, B = HL.at[jA, :, :, chunk(t)], HL.at[jB, :, :, chunk(t)]
        got(B, ("hb", t), zeta == 0)
        got(B, ("hB", t), zeta == 3)
        got(A, ("hA", t), zeta == 3)
        send(HL.at[1 - k, :, :, chunk(t)], HP.at[:, :, chunk(t)], ("hd", t), dev(r_=rp))
        out(HL.at[k, :, :, chunk(t)], ho.at[:, k, :, chunk(t)], "ho", t)

    outs = []

    def out(src, dst, *name):
        cp = local(src, dst, *name)
        cp.start()
        outs.append(cp)

    target = jnp.where(y == 0, k, 1 - k)

    def piece(u):
        t, ln = u // 2, RBS[u // 2] // 2
        return OFF[t] + u % 2 * ln, ln

    def dx_part(t, i):
        q = (r, rp, ro, rx)[i]
        theirs = DB.at[q, :, chunk(t)]
        if i == 1:
            got(theirs, ("dbd", t))
        if i == 3:
            got(theirs, ("dbf", t))
            out(DB.at[:, :, chunk(t)], dbo.at[:, :, chunk(t)], "dbo", t)
        sl = slice(OFF[t], OFF[t] + RBS[t])

        def go():
            d = lax.dot_general(DB[q, :, sl].reshape(4 * RBS[t], 2 * fq), WV[q], NT_DIMS, preferred_element_type=F32).reshape(2, 2, RBS[t], cm)
            DXS[:, :, sl] = d if i == 0 else DXS[:, :, sl] + d

        go()
        if i < 3:
            return
        if t < CHAIN:
            for u in (2 * t, 2 * t + 1):
                rs = pl.ds(*piece(u))
                send(DXS.at[:, :, rs], DXA.at[:, :, rs], ("dxa", u), dev(z_=zb), zeta == 3, False)
                send(DXS.at[:, :, rs], DXM.at[:, :, rs], ("dxm", u), dev(z_=zf), both(zeta == 0, target == 1))
        else:
            send(DXS.at[1 - c, :, chunk(t)], DXA.at[0, :, chunk(t)], ("dx1", t), dev(z_=zm))

    def dx_add(u, cond, parts):
        off, ln = piece(u)
        sl = slice(off, off + ln)

        def go():
            for ref in parts:
                DXS[:, :, sl] += ref[:, :, sl]

        pl.when(cond)(go)

    def dx_step(u, at):
        rs = pl.ds(*piece(u))
        on = zeta == at
        goes = both(on, at > target) if at else both(on, target < 0)
        got(DXA.at[:, :, rs], ("dxa", u), both(on, at >= target))
        if at == 1:
            got(DXM.at[:, :, rs], ("dxm", u), both(on, target == 1))
            dx_add(u, both(on, target == 1), (DXA, DXM))
            dx_add(u, both(on, target == 0), (DXA,))
        else:
            dx_add(u, both(on, at >= target), (DXA,))
        if at:
            send(DXS.at[:, :, rs], DXA.at[:, :, rs], ("dxa", u), dev(z_=zb), goes, both(zeta >= 1, zeta > target) if at == 1 else False)

    def dx_spread(u):
        off, ln = piece(u)
        sl, rs = slice(off, off + ln), pl.ds(off, ln)

        @pl.when(diag)
        def _():
            DXF.__setitem__((slice(None), slice(None), sl), DXS[:, :, sl].astype(BF16))

        for k2, y2, i in ((1 - k, y, 0), (k, 1 - y, 1), (1 - k, 1 - y, 2)):
            send(DXF.at[k2, y2, rs], DXR.at[rs], ("dxf", u, i), dev(r_=2 * y2 + k2), diag)

    def dx_half(t):
        sl = slice(OFF[t], OFF[t] + RBS[t])
        got(DXA.at[0, :, chunk(t)], ("dx1", t))

        def go():
            DXS[c, :, sl] += DXA[0, :, sl]

        go()
        send(DXS.at[c, 1 - pr, chunk(t)], DXM.at[0, 0, chunk(t)], ("dx2", t), dev(z_=zt))

    def dx_quarter(t):
        sl = slice(OFF[t], OFF[t] + RBS[t])
        got(DXM.at[0, 0, chunk(t)], ("dx2", t))

        def go():
            DXF[k, y, sl] = (DXS[c, pr, sl] + DXM[0, 0, sl]).astype(BF16)

        go()
        send(DXF.at[k, y, chunk(t)], DXR.at[chunk(t)], ("dxt", t), dev(z_=r, r_=z), jnp.logical_not(diag))

    def dy_send():
        send(gy_hbm, DY.at[c, k, y], ("dyy",), dev(r_=ro))

    def w_swap():
        for m, w in enumerate((wg_hbm, wu_hbm)):
            for s in range(2):
                send(w.at[:, pl.ds(pl.multiple_of((1 - k + 2 * s) * fq, 128), fq)], WP.at[s, :, pl.ds(m * fq, fq)], ("w", m, s), dev(r_=rp))

    def h_take(t):
        got(HP.at[:, :, chunk(t)], ("hd", t))
        out(HP.at[:, :, chunk(t)], ho.at[:, 1 - k, :, chunk(t)], "hp", t)

    def dx_take(t):
        sl = slice(OFF[t], OFF[t] + RBS[t])
        zk, zy = z % 2, z // 2

        @pl.when(diag)
        def _():
            DXR.__setitem__(sl, DXF[k, y, sl])

        if t < CHAIN:
            for u in (2 * t, 2 * t + 1):
                rs = pl.ds(*piece(u))
                got(DXR.at[rs], ("dxf", u, 0), both(zk != k, zy == y))
                got(DXR.at[rs], ("dxf", u, 1), both(zk == k, zy != y))
                got(DXR.at[rs], ("dxf", u, 2), both(zk != k, zy != y))
        else:
            got(DXR.at[chunk(t)], ("dxt", t), jnp.logical_not(diag))

    def out_early():
        XT.__setitem__(Ellipsis, XG[k].reshape(4 * rows, cm).T)
        out(XT, xo, "xo")
        out(DY.at[c], dyo, "dyo")

    i0, i1, i2, i3, i4, i5, i6, i7, i8, i9 = range(10)
    yes, no = True, False
    wo_near(i1, home)
    wo_far(i0, i1, home)
    x_send(i0)
    wo_near(i2, home)
    wo_far(i1, i0, home)
    dy_send()
    wo_far(i2, i1, home)
    wo_far(i0, i1, away)
    wo_relay(i0, home)
    x_send(i1)
    wo_near(i0, away)
    wo_far(i1, i1, away)
    w_swap()
    wo_pass(i2, i1, home)
    x_step(i0, i1, i1)
    wo_relay(i2, home)
    x_step(i0, i1, i0)
    x_step(i1, i1, i1)
    x_step(i1, i1, i0)
    wo_near(i1, away)
    wo_pass(i3, i0, away)
    wo_far(i0, i0, away)
    x_step(i0, i2, i1)
    weights_here()
    wo_far(i0, i0, home)
    x_step(i0, i2, i0)
    wo_relay(i0, away)
    x_step(i1, i2, i0)
    x_step(i1, i2, i1)
    dy_pass()
    wo_far(i2, i0, home)
    x_step(i0, i3, i0)
    wo_far(i1, i1, home)
    wo_pass(i1, i0, home)
    wo_far(i1, i0, away)
    wo_near(i0, home)
    wo_near(i2, away)
    x_step(i1, i3, i0)
    wo_pass(i1, i1, home)
    wo_pass(i3, i0, home)
    wo_pass(i2, i0, home)
    wo_pass(i1, i2, away)
    wo_relay(i1, away)
    x_step(i0, i3, i1)
    x_give(i0)
    x_take(i0)
    x_step(i1, i3, i1)
    wo_pass(i1, i1, away)
    ab_mirror(i1)
    x_give(i1)
    x_take(i1)
    ab_mirror(i2)
    ab_mirror(i0, home, yes)
    wo_pass(i1, i0, away)
    wo_far(i2, i0, away)
    wo_pass(i2, i0, away)
    dy_give()
    wo_pass(i3, i1, home)
    wo_far(i2, i1, away)
    dy_take()
    dh_mirror(i0)
    wo_pass(i1, i2, home)
    wo_pass(i2, i1, away)
    dh_mirror(i1)
    wo_relay(i1, home)
    wo_relay(i2, away)
    wo_pass(i2, i2, away)
    finish_ab(i2)
    wo_pass(i3, i2, home)
    h_start(i2)
    dh_own(i0)
    wo_pass(i3, i2, away)
    dh_mirror(i2)
    ab_mirror(i0, away, no)
    finish_ab(i1)
    wo_pass(i2, i2, home)
    ab_mirror(i3)
    out_early()
    dh_own(i2)
    wo_pass(i3, i1, away)
    finish_ab(i0)
    dh_own(i1)
    finish_dh(i0)
    finish_dh(i1)
    h_start(i1)
    finish_ab(i3)
    dx_part(i1, i0)
    dx_part(i0, i0)
    h_start(i0)
    h_pass(i2, i0)
    finish_dh(i2)
    relay_db(i0)
    dx_part(i0, i1)
    finish_dh(i3)
    h_pass(i2, i1)
    dx_part(i0, i2)
    dx_part(i0, i3)
    dx_part(i1, i1)
    relay_db(i1)
    h_pass(i1, i0)
    h_start(i3)
    dx_part(i1, i2)
    dx_part(i1, i3)
    dx_part(i2, i0)
    h_pass(i0, i1)
    dx_step(i0, i2)
    h_pass(i0, i0)
    dx_part(i2, i1)
    relay_db(i2)
    h_pass(i1, i1)
    dx_part(i2, i2)
    dx_part(i3, i0)
    dx_step(i1, i2)
    dx_step(i0, i1)
    dx_part(i2, i3)
    dx_step(i1, i1)
    relay_db(i3)
    dx_step(i0, i0)
    h_pass(i2, i2)
    dx_part(i3, i1)
    dx_step(i2, i2)
    dx_step(i2, i1)
    dx_part(i3, i2)
    dx_part(i3, i3)
    dx_step(i2, i0)
    h_pass(i3, i0)
    dx_spread(i2)
    dx_step(i3, i2)
    dx_step(i3, i1)
    dx_step(i1, i0)
    h_pass(i0, i2)
    h_pass(i3, i1)
    dx_step(i4, i2)
    dx_step(i5, i2)
    dx_step(i3, i0)
    dx_step(i4, i1)
    dx_spread(i1)
    dx_half(i3)
    dx_step(i4, i0)
    h_last(i2)
    dx_spread(i0)
    dx_spread(i3)
    dx_spread(i4)
    dx_step(i5, i1)
    dx_step(i5, i0)
    h_last(i0)
    dx_spread(i5)
    h_pass(i1, i2)
    dx_quarter(i3)
    h_pass(i3, i2)
    h_last(i1)
    dx_take(i1)
    dx_take(i2)
    h_take(i0)
    h_take(i1)
    h_take(i2)
    dx_take(i3)
    h_last(i3)
    dx_take(i0)
    h_take(i3)

    out(DXR, dxo, "dxo")
    for cond, cp in pending:
        if cond is None:
            cp.wait_send()
        else:
            pl.when(cond)(cp.wait_send)
    for cp in outs:
        cp.wait()


def dw_kernel(x_hbm, dy_hbm, db_hbm, h_hbm, dx_hbm, dwg, dwu, dwo, dxo, XT, DY, DB, H, OA, OB, in_sem, out_sem):
    fq = H.shape[-1]
    loads = [pltpu.make_async_copy(x_hbm, XT, in_sem.at[0])]
    loads += [pltpu.make_async_copy(db_hbm.at[q], DB.at[q], in_sem.at[1 + q]) for q in range(4)]
    loads += [pltpu.make_async_copy(dy_hbm, DY, in_sem.at[5])]
    loads += [pltpu.make_async_copy(h_hbm.at[q], H.at[q], in_sem.at[6 + q]) for q in range(4)]
    for cp in loads:
        cp.start()
    outs = []

    def put(src, dst):
        cp = pltpu.make_async_copy(src, dst, out_sem.at[len(outs)])
        cp.start()
        outs.append(cp)

    loads[0].wait()
    for q in range(4):
        loads[1 + q].wait()
        OA[q] = jnp.dot(XT[...], DB[q], preferred_element_type=F32)
        for m, dst in enumerate((dwg, dwu)):
            put(OA.at[q, :, pl.ds(m * fq, fq)], dst.at[:, pl.ds(q * fq, fq)])
    loads[5].wait()
    for q in range(4):
        loads[6 + q].wait()
        OB[q] = lax.dot_general(H[q], DY[...], TN_DIMS, preferred_element_type=F32)
        put(OB.at[q], dwo.at[pl.ds(q * fq, fq)])
    dxo[...] = dx_hbm[...]
    for cp in outs:
        cp.wait()


def solution(mesh):
    act_spec = P(("dp", "row"), "col")
    weight_spec = P("row", "col")

    def block_backward(x_blk, gy_blk, gate_blk, up_blk, out_blk):
        rows, dm = x_blk.shape
        ff = gate_blk.shape[1]
        fq, tok = ff // 4, 4 * rows
        vm = pltpu.VMEM
        xg, dyg, dbg, hg, dxg = pl.pallas_call(
            lambda *refs: comm_kernel(rows, dm, ff, *refs),
            out_shape=[
                jax.ShapeDtypeStruct((dm, tok), BF16),
                jax.ShapeDtypeStruct((2, 2, rows, dm), BF16),
                jax.ShapeDtypeStruct((4, 4, rows, 2 * fq), BF16),
                jax.ShapeDtypeStruct((2, 2, 4, rows, fq), BF16),
                jax.ShapeDtypeStruct((rows, dm), BF16),
            ],
            in_specs=[ANY] * 5,
            out_specs=[ANY] * 5,
            scratch_shapes=[
                vm((2, 2, 2, rows, dm), BF16),
                vm((2, rows, dm), BF16),
                vm((2, 2, 2, rows, dm), BF16),
                vm((4, dm, 2 * fq), BF16),
                vm((2, dm, 2 * fq), BF16),
                vm((2, fq, 2 * dm), BF16),
                vm((fq, dm // 2), BF16),
                vm((4, rows, 2 * fq), F32),
                vm((4, rows, 2 * fq), F32),
                vm((4, max(RBS), 2 * fq), F32),
                vm((4, rows, fq), F32),
                vm((4, rows, fq), F32),
                vm((4, rows, fq), F32),
                vm((4, 4, rows, 2 * fq), BF16),
                vm((3, 2, 4, rows, fq), BF16),
                vm((2, 4, rows, fq), BF16),
                vm((2, 2, rows, dm), F32),
                vm((2, 2, rows, dm), F32),
                vm((2, 2, rows, dm), F32),
                vm((2, 2, rows, dm), BF16),
                vm((rows, dm), BF16),
                vm((dm, tok), BF16),
                pltpu.SemaphoreType.DMA((N_SEND,)),
                pltpu.SemaphoreType.DMA((N_RECV,)),
                pltpu.SemaphoreType.DMA((N_LOCAL,)),
            ],
            compiler_params=pltpu.CompilerParams(collective_id=0, has_side_effects=True, vmem_limit_bytes=63 * 1024 * 1024),
            name="comm",
        )(x_blk, gy_blk, gate_blk, up_blk, out_blk)
        whole = pl.BlockSpec(memory_space=vm)
        dw_gate, dw_up, dw_out, grad_x = pl.pallas_call(
            dw_kernel,
            out_shape=[
                jax.ShapeDtypeStruct((dm, ff), F32),
                jax.ShapeDtypeStruct((dm, ff), F32),
                jax.ShapeDtypeStruct((ff, dm), F32),
                jax.ShapeDtypeStruct((rows, dm), BF16),
            ],
            in_specs=[ANY] * 4 + [whole],
            out_specs=[ANY] * 3 + [whole],
            scratch_shapes=[
                vm((dm, tok), BF16), vm((tok, dm), BF16),
                vm((4, tok, 2 * fq), BF16), vm((4, tok, fq), BF16),
                vm((4, dm, 2 * fq), F32), vm((4, fq, dm), F32),
                pltpu.SemaphoreType.DMA((10,)), pltpu.SemaphoreType.DMA((12,)),
            ],
            compiler_params=pltpu.CompilerParams(vmem_limit_bytes=60 * 1024 * 1024),
            name="dw",
        )(xg, dyg.reshape(tok, dm), dbg.reshape(4, tok, 2 * fq), hg.reshape(4, tok, fq), dxg)
        return grad_x, dw_gate, dw_up, dw_out

    return jax.shard_map(block_backward, mesh=mesh, in_specs=(act_spec, act_spec, weight_spec, weight_spec, weight_spec), out_specs=(act_spec, act_spec, act_spec, act_spec), check_vma=False)
```

```python
import math
import jax
import jax.numpy as jnp
from jax import lax
from jax.experimental import pallas as pl
from jax.experimental.pallas import tpu as pltpu
from jax.sharding import PartitionSpec as P

GELU_SCALE = math.sqrt(2.0 / math.pi)
F32, BF16 = jnp.float32, jnp.bfloat16
MESH = pl.DeviceIdType.MESH
ANY = pl.BlockSpec(memory_space=pl.ANY)
NT_DIMS = (((1,), (1,)), ((), ()))
TN_DIMS = (((0,), (0,)), ((), ()))
RBS = (32, 32, 32, 32)
NCH = len(RBS)
CHAIN = 3
OFF = tuple(sum(RBS[:t]) for t in range(NCH))
PIECES = tuple((t, OFF[t] + h * n, n) for t in range(CHAIN) for n in (RBS[t] // (2 if RBS[t] % 32 == 0 else 1),) for h in range(RBS[t] // n))
X_CUT = ((0, 64), (64, 64))
N_CUT = ((0, 256), (256, 384))
NS = range(len(N_CUT))
N_SEND, N_RECV, N_LOCAL = 240, 240, 64


def gelu_pair(pre_f32):
    inner_arg = GELU_SCALE * (pre_f32 + 0.044715 * pre_f32 * pre_f32 * pre_f32)
    tanh_val = jnp.tanh(inner_arg)
    gelu_val = 0.5 * pre_f32 * (1.0 + tanh_val)
    gelu_der = 0.5 * (1.0 + tanh_val) + 0.5 * pre_f32 * (1.0 - tanh_val * tanh_val) * GELU_SCALE * (1.0 + 3.0 * 0.044715 * pre_f32 * pre_f32)
    return gelu_val, gelu_der


class Slots:
    def __init__(self, ref, size):
        self.ref, self.size, self.names, self.used = ref, size, {}, 0

    def __call__(self, *name, off=None):
        if name not in self.names:
            self.names[name] = self.used
            self.used += 1 if off is None else 4
            assert self.used <= self.size
        i = self.names[name]
        return self.ref.at[i if off is None else i + off]


def comm_kernel(rows, dm, ff,
                x_hbm, gy_hbm, wg_hbm, wu_hbm, wo_hbm,
                xo, dyo, dbo, ho, dxo,
                XG, XR, DY, WV, WP, WO, WR, AS, AR, AO, DO, DB, HL, HP, DXS, DXA, DXM, DXF, DXR, XT,
                send_ref, recv_ref, local_ref):
    fq = ff // 4
    cm = dm
    S, R, L = Slots(send_ref, N_SEND), Slots(recv_ref, N_RECV), Slots(local_ref, N_LOCAL)
    p, z, r = lax.axis_index("dp"), lax.axis_index("col"), lax.axis_index("row")
    y, k = r // 2, r % 2
    pr, c = z // 2, z % 2
    zm, zt = z + 1 - 2 * c, z + 2 - 4 * pr
    home, away = y == pr, y != pr
    zeta = jnp.where(y == 0, z, 3 - z)
    zf, zb = z + 1 - 2 * y, z - 1 + 2 * y
    z2 = jnp.where(y == 0, 2, 1)
    jA, jB = y, 1 - y
    ro, rp = 2 * (1 - y) + k, 2 * y + 1 - k
    rx = 2 * (1 - y) + 1 - k
    diag = z == r

    def both(a, b):
        return jnp.logical_and(a, b)

    def dev(z_=z, r_=r, p_=p):
        return {"dp": p_, "col": z_, "row": r_}

    pending = []

    def remote(src, dst, name, to, off=None):
        return pltpu.make_async_remote_copy(src_ref=src, dst_ref=dst, send_sem=S(*name), recv_sem=R(*name, off=off), device_id=to, device_id_type=MESH)

    def send(src, dst, name, to, cond=None, last=None, off=None):
        cp = remote(src, dst, name, to, off)
        if cond is None:
            cp.start()
        else:
            pl.when(cond)(cp.start)
        if last is not False:
            pending.append((cond if last is None else None if last is True else last, cp))

    def got(dst, name, cond=None, off=None):
        cp = remote(dst, dst, name, dev(p_=1 - p), off)
        if cond is None:
            cp.wait_recv()
        else:
            pl.when(cond)(cp.wait_recv)

    def local(src, dst, *name):
        return pltpu.make_async_copy(src, dst, L(*name))

    barrier = pltpu.get_barrier_semaphore()
    peers = [dev(p_=1 - p)] + [dev(z_=(z + dz) % 4, r_=(r + dr) % 4) for dz in range(4) for dr in range(4) if dz or dr]
    for peer in peers:
        pl.semaphore_signal(barrier, inc=1, device_id=peer, device_id_type=MESH)

    lx = local(x_hbm, XG.at[c, k, y], "x")
    pl.when(home)(lx.start)
    ldy = local(gy_hbm, DY.at[z, k, y], "dy")
    ldy.start()
    lw = []
    for m, w in enumerate((wg_hbm, wu_hbm)):
        for q in range(4):
            cp = local(w.at[:, pl.ds(q * fq, fq)], WV.at[q, :, pl.ds(m * fq, fq)], "w", m, q)
            cp.start()
            lw.append(cp)

    half = cm // 2
    pcols = pl.ds(pl.multiple_of(p * half, 512), half)
    line = (z, zm, zt, zt + 1 - 2 * (zt % 2))

    def wo_cut(q, n, cols):
        off, ln = N_CUT[n]
        return wo_hbm.at[pl.ds(pl.multiple_of(q * fq + off, 128), ln), cols]

    def wo_slot(n, src_z, start, width):
        off, ln = N_CUT[n]
        return WO.at[pl.ds(off, ln), pl.ds(pl.multiple_of(src_z * cm + start, 512), width)]

    lwo = []
    for n in NS:
        cp = local(wo_cut(r, n, pl.ds(0, cm)), wo_slot(n, z, 0, cm), "wo", n)
        pl.when(diag)(cp.start)
        lwo.append(cp)
    pl.semaphore_wait(barrier, len(peers))

    def chunk(t):
        return pl.ds(OFF[t], RBS[t])

    def x_place(src_z, ts, cond):
        mine = src_z // 2 == y
        return ((XG.at[src_z % 2, k, y, ts], both(cond, mine)), (XR.at[src_z % 2, ts], both(cond, jnp.logical_not(mine))))

    def x_send(th):
        ts = pl.ds(*X_CUT[th])
        for name, to, cond in (("xr", z + 1, z < 3), ("xl", z - 1, z > 0)):
            for dst, ok in x_place(z, ts, cond):
                send(x_hbm.at[ts], dst, (name, th, 1), dev(z_=to), ok)
        send(x_hbm.at[ts], XG.at[c, k, y, ts], ("xy", th, 0), dev(r_=ro), away)

    def x_step(th, d, left):
        ts = pl.ds(*X_CUT[th])
        src_z, to = (z + d, z - 1) if left else (z - d, z + 1)
        here = src_z <= 3 if left else src_z >= 0
        more = both(here, to >= 0 if left else to <= 3)
        name = "xl" if left else "xr"
        for ref, ok in x_place(src_z, ts, here):
            got(ref, (name, th, d), ok)
            if d < 3:
                send(ref, ref, (name, th, d + 1), dev(z_=to), both(ok, more))
        ref, ok = x_place(src_z, ts, here)[1]
        same = src_z % 2 == c
        send(ref, XG.at[src_z % 2, k, y, ts], ("xy", th, 0), dev(r_=ro), both(ok, same))
        send(ref, XG.at[src_z % 2, k, y, ts], ("xy", th, 1), dev(r_=ro), both(ok, jnp.logical_not(same)))

    def x_give(th):
        ts = pl.ds(*X_CUT[th])
        if th == 0:
            pl.when(home)(lx.wait)
        got(XG.at[c, k, 1 - y, ts], ("xy", th, 0))
        got(XG.at[1 - c, k, 1 - y, ts], ("xy", th, 1))
        send(XG.at[:, k, :, ts], XG.at[:, k, :, ts], ("xd", th), dev(r_=rp))

    def x_take(th):
        got(XG.at[:, 1 - k, :, pl.ds(*X_CUT[th])], ("xd", th))

    def dy_send():
        send(gy_hbm, DY.at[z, k, y], ("dyy",), dev(r_=ro))

    def dy_pass():
        ldy.wait()
        mine = DY.at[z, k]
        got(DY.at[z, k, 1 - y], ("dyy",))
        send(mine, mine, ("dr", 1), dev(z_=z + 1), z < 3)
        send(mine, mine, ("dl", 1), dev(z_=z - 1), z > 0)
        send(mine, mine, ("dyd", 0, 0), dev(r_=rp))

    def dy_from(d, left):
        src_z = z + d if left else z - d
        return src_z, src_z <= 3 if left else src_z >= 0

    def dy_step(d, left):
        src_z, here = dy_from(d, left)
        to = z - 1 if left else z + 1
        more = to >= 0 if left else to <= 3
        name = "dl" if left else "dr"
        theirs = DY.at[src_z, k]
        got(theirs, (name, d), here)
        if d < 3:
            send(theirs, theirs, (name, d + 1), dev(z_=to), both(here, more))
        send(theirs, theirs, ("dyd", d, left), dev(r_=rp), here)

    def dy_take():
        got(DY.at[z, 1 - k], ("dyd", 0, 0))
        for d in range(1, 4):
            for left in range(2):
                src_z, here = dy_from(d, left)
                got(DY.at[src_z, 1 - k], ("dyd", d, left), here)

    def wo_near(n):
        send(wo_cut(rp, n, pl.ds(0, cm)), wo_slot(n, z, 0, cm), ("wn", n), dev(r_=rp), diag)

    def wo_own(n):
        for k2 in range(2):
            q = 2 * y + k2
            send(wo_cut(q, n, pcols), wo_slot(n, z, p * half, half), ("wz", n, k2), dev(z_=r, r_=q), jnp.logical_not(diag), None, z)

    def wo_cross(n):
        off, ln = N_CUT[n]
        for k2 in range(2):
            q = 2 * (1 - y) + k2
            send(wo_cut(q, n, pcols), wo_slot(n, z, p * half, half), ("wd", n, k2), dev(r_=q), diag)
            send(wo_cut(q, n, pcols), WR.at[k2, pl.ds(off, ln)], ("wr", n, k2), dev(r_=ro), jnp.logical_not(diag))

    def wo_relay(n):
        off, ln = N_CUT[n]
        for k2 in range(2):
            got(WR.at[k2, pl.ds(off, ln)], ("wr", n, k2), z != ro)
            send(WR.at[k2, pl.ds(off, ln)], wo_slot(n, z, p * half, half), ("wv", n, k2), dev(z_=ro, r_=2 * y + k2), z != ro, None, z)

    def wo_pass(n, i):
        src_z = line[i]
        mine = wo_slot(n, src_z, p * half, half)
        for k2 in range(2):
            if i == 0:
                got(mine, ("wd", n, k2), both(away, k == k2))
            else:
                got(mine, ("wz", n, k2), both(home, k == k2), src_z)
                got(mine, ("wv", n, k2), both(away, k == k2), src_z)
        send(mine, mine, ("wx", n, i), dev(p_=1 - p), away if i == 0 else None)

    def dh_part(n):
        off, ln = N_CUT[n]
        pl.when(both(home, diag))(lwo[n].wait)
        got(wo_slot(n, z, 0, cm), ("wn", n), both(home, jnp.logical_not(diag)))
        for i in range(4):
            got(wo_slot(n, line[i], (1 - p) * half, half), ("wx", n, i), away if i == 0 else None)

        def go():
            for j in range(4):
                d = lax.dot_general(DY[j].reshape(4 * rows, cm), WO[off:off + ln, j * cm:(j + 1) * cm], NT_DIMS, preferred_element_type=F32).reshape(4, rows, ln)
                DO[:, :, off:off + ln] = d if j == 0 else DO[:, :, off:off + ln] + d

        go()

    def ab_part(s, t):
        tc = 4 * RBS[t]
        own = jnp.dot(XG[k, :, :, OFF[t]:OFF[t] + RBS[t]].reshape(tc, cm), WV[k + 2 * s], preferred_element_type=F32)
        other = jnp.dot(XG[1 - k, :, :, OFF[t]:OFF[t] + RBS[t]].reshape(tc, cm), WP[s], preferred_element_type=F32)
        return (own + other).reshape(4, RBS[t], 2 * fq)

    def ab_mirror(t, cond=None, last=True):
        def go():
            AS[:, OFF[t]:OFF[t] + RBS[t]] = ab_part(1 - y, t)

        go() if cond is None else pl.when(cond)(go)
        send(AS.at[:, chunk(t)], AR.at[:, chunk(t)], ("ab", t), dev(r_=ro), cond, last)

    def weights_here():
        for cp in lw:
            cp.wait()
        for m in range(2):
            for s in range(2):
                got(WP.at[s, :, pl.ds(m * fq, fq)], ("w", m, s))

    hs = jnp.where(home, c, 2)

    def row_blocks(t, fn):
        nb = RBS[t] // 16

        def body(i, _):
            fn(i // nb, pl.ds(pl.multiple_of(OFF[t] + i % nb * 16, 16), 16))
            return 0

        lax.fori_loop(0, 4 * nb, body, 0)

    def finish_ab(t):
        def own():
            AO[:, :RBS[t]] = ab_part(y, t)

        own()
        got(AR.at[:, chunk(t)], ("ab", t))

        def body(o, rs):
            ra = pl.ds(pl.multiple_of(rs.start - OFF[t], 16), 16)
            a = (AO[o, ra, :fq] + AR[o, rs, :fq]).astype(BF16).astype(F32)
            b = (AO[o, ra, fq:] + AR[o, rs, fq:]).astype(BF16).astype(F32)
            g, gd = gelu_pair(a)
            HL[hs, y, o, rs] = (g * b).astype(BF16)
            AR[o, rs, :fq] = b * gd
            AR[o, rs, fq:] = g

        row_blocks(t, body)
        send(HL.at[2, y, :, chunk(t)], HL.at[c, y, :, chunk(t)], ("hy", t), dev(r_=ro), away)

    def finish_dh(t):
        def body(o, rs):
            dh = DO[o, rs]
            DB[r, o, rs, :fq] = (dh * AR[o, rs, :fq]).astype(BF16)
            DB[r, o, rs, fq:] = (dh * AR[o, rs, fq:]).astype(BF16)

        row_blocks(t, body)
        mine = DB.at[r, :, chunk(t)]
        send(mine, mine, ("dby", t), dev(r_=ro))
        send(mine, mine, ("dbd", t), dev(r_=rp))

    def relay_db(t):
        theirs = DB.at[ro, :, chunk(t)]
        got(theirs, ("dby", t))
        send(theirs, theirs, ("dbf", t), dev(r_=rp))

    def h_start(t):
        A, B = HL.at[jA, :, :, chunk(t)], HL.at[jB, :, :, chunk(t)]
        got(HL.at[c, 1 - y, :, chunk(t)], ("hy", t), home)
        send(A, A, ("hA", t), dev(z_=zf), zeta == 0, zeta <= 2)
        send(B, B, ("hB", t), dev(z_=zf), zeta == 1, both(zeta >= 1, zeta <= 2))
        send(B, B, ("hb", t), dev(z_=zb), zeta == 1)

    def h_pass(t, i):
        if i == 0:
            B = HL.at[jB, :, :, chunk(t)]
            got(B, ("hB", t), zeta == 2)
            send(B, B, ("hB", t), dev(z_=zf), zeta == 2, False)
        else:
            A = HL.at[jA, :, :, chunk(t)]
            got(A, ("hA", t), zeta == i)
            send(A, A, ("hA", t), dev(z_=zf), zeta == i, False)

    def h_last(t):
        A, B = HL.at[jA, :, :, chunk(t)], HL.at[jB, :, :, chunk(t)]
        got(B, ("hb", t), zeta == 0)
        got(B, ("hB", t), zeta == 3)
        got(A, ("hA", t), zeta == 3)
        send(HL.at[1 - k, :, :, chunk(t)], HP.at[:, :, chunk(t)], ("hd", t), dev(r_=rp))
        out(HL.at[k, :, :, chunk(t)], ho.at[:, k, :, chunk(t)], "ho", t)

    outs = []

    def out(src, dst, *name):
        cp = local(src, dst, *name)
        cp.start()
        outs.append(cp)

    target = jnp.where(y == 0, k, 1 - k)

    def piece(u):
        return PIECES[u][1:]

    def pieces(t):
        return [u for u in range(len(PIECES)) if PIECES[u][0] == t]

    def dx_part(t, i):
        q = (r, rp, ro, rx)[i]
        theirs = DB.at[q, :, chunk(t)]
        if i == 1:
            got(theirs, ("dbd", t))
        if i == 3:
            got(theirs, ("dbf", t))
            out(DB.at[:, :, chunk(t)], dbo.at[:, :, chunk(t)], "dbo", t)
        sl = slice(OFF[t], OFF[t] + RBS[t])

        def go():
            d = lax.dot_general(DB[q, :, sl].reshape(4 * RBS[t], 2 * fq), WV[q], NT_DIMS, preferred_element_type=F32).reshape(2, 2, RBS[t], cm)
            DXS[:, :, sl] = d if i == 0 else DXS[:, :, sl] + d

        go()
        if i < 3:
            return
        if t < CHAIN:
            for u in pieces(t):
                rs = pl.ds(*piece(u))
                send(DXS.at[:, :, rs], DXA.at[:, :, rs], ("dxa", u), dev(z_=zb), zeta == 3, False)
                send(DXS.at[:, :, rs], DXM.at[:, :, rs], ("dxm", u), dev(z_=zf), both(zeta == 0, target == 1))
        else:
            send(DXS.at[1 - c, :, chunk(t)], DXA.at[0, :, chunk(t)], ("dx1", t), dev(z_=zm))

    def dx_add(u, cond, parts):
        off, ln = piece(u)
        sl = slice(off, off + ln)

        def go():
            for ref in parts:
                DXS[:, :, sl] += ref[:, :, sl]

        pl.when(cond)(go)

    def dx_step(u, at):
        rs = pl.ds(*piece(u))
        on = zeta == at
        goes = both(on, at > target) if at else both(on, target < 0)
        got(DXA.at[:, :, rs], ("dxa", u), both(on, at >= target))
        if at == 1:
            got(DXM.at[:, :, rs], ("dxm", u), both(on, target == 1))
            dx_add(u, both(on, target == 1), (DXA, DXM))
            dx_add(u, both(on, target == 0), (DXA,))
        else:
            dx_add(u, both(on, at >= target), (DXA,))
        if at:
            send(DXS.at[:, :, rs], DXA.at[:, :, rs], ("dxa", u), dev(z_=zb), goes, both(zeta >= 1, zeta > target) if at == 1 else False)

    def dx_spread(u):
        off, ln = piece(u)
        sl, rs = slice(off, off + ln), pl.ds(off, ln)

        @pl.when(diag)
        def _():
            DXF.__setitem__((slice(None), slice(None), sl), DXS[:, :, sl].astype(BF16))

        for k2, y2, i in ((1 - k, y, 0), (k, 1 - y, 1), (1 - k, 1 - y, 2)):
            send(DXF.at[k2, y2, rs], DXR.at[rs], ("dxf", u, i), dev(r_=2 * y2 + k2), diag)

    def dx_half(t):
        sl = slice(OFF[t], OFF[t] + RBS[t])
        got(DXA.at[0, :, chunk(t)], ("dx1", t))

        def go():
            DXS[c, :, sl] += DXA[0, :, sl]

        go()
        send(DXS.at[c, 1 - pr, chunk(t)], DXM.at[0, 0, chunk(t)], ("dx2", t), dev(z_=zt))

    def dx_quarter(t):
        sl = slice(OFF[t], OFF[t] + RBS[t])
        got(DXM.at[0, 0, chunk(t)], ("dx2", t))

        def go():
            DXF[k, y, sl] = (DXS[c, pr, sl] + DXM[0, 0, sl]).astype(BF16)

        go()
        send(DXF.at[k, y, chunk(t)], DXR.at[chunk(t)], ("dxt", t), dev(z_=r, r_=z), jnp.logical_not(diag))

    def w_swap():
        for m, w in enumerate((wg_hbm, wu_hbm)):
            for s in range(2):
                send(w.at[:, pl.ds(pl.multiple_of((1 - k + 2 * s) * fq, 128), fq)], WP.at[s, :, pl.ds(m * fq, fq)], ("w", m, s), dev(r_=rp))

    def h_take(t):
        got(HP.at[:, :, chunk(t)], ("hd", t))
        out(HP.at[:, :, chunk(t)], ho.at[:, 1 - k, :, chunk(t)], "hp", t)

    def dx_take(t):
        sl = slice(OFF[t], OFF[t] + RBS[t])
        zk, zy = z % 2, z // 2

        @pl.when(diag)
        def _():
            DXR.__setitem__(sl, DXF[k, y, sl])

        if t < CHAIN:
            for u in pieces(t):
                rs = pl.ds(*piece(u))
                got(DXR.at[rs], ("dxf", u, 0), both(zk != k, zy == y))
                got(DXR.at[rs], ("dxf", u, 1), both(zk == k, zy != y))
                got(DXR.at[rs], ("dxf", u, 2), both(zk != k, zy != y))
        else:
            got(DXR.at[chunk(t)], ("dxt", t), jnp.logical_not(diag))

    def out_early():
        XT.__setitem__(Ellipsis, XG[k].reshape(4 * rows, cm).T)
        out(XT, xo, "xo")
        out(DY.at[z], dyo, "dyo")

    i0, i1, i2, i3, i4, i5, i6, i7, i8, i9 = range(10)
    yes, no = True, False
    x_send(i0)
    dy_send()
    wo_cross(i1)
    wo_cross(i0)
    x_send(i1)
    x_step(i0, i1, i1)
    x_step(i0, i1, i0)
    x_step(i1, i1, i1)
    x_step(i0, i2, i0)
    x_step(i0, i3, i0)
    x_step(i1, i1, i0)
    x_step(i0, i2, i1)
    dy_pass()
    x_step(i1, i2, i0)
    wo_own(i1)
    wo_near(i1)
    w_swap()
    wo_relay(i1)
    x_step(i0, i3, i1)
    x_step(i1, i2, i1)
    x_give(i0)
    x_step(i1, i3, i1)
    dy_step(i1, i1)
    wo_near(i0)
    dy_step(i1, i0)
    wo_own(i0)
    wo_pass(i0, i0)
    wo_relay(i0)
    x_step(i1, i3, i0)
    weights_here()
    x_take(i0)
    ab_mirror(i0, home, yes)
    ab_mirror(i1)
    wo_pass(i1, i0)
    ab_mirror(i0, away, no)
    x_give(i1)
    x_take(i1)
    ab_mirror(i2)
    wo_pass(i1, i1)
    wo_pass(i1, i3)
    wo_pass(i1, i2)
    finish_ab(i0)
    dy_step(i2, i1)
    finish_ab(i1)
    wo_pass(i0, i1)
    dy_step(i2, i0)
    wo_pass(i0, i3)
    finish_ab(i2)
    ab_mirror(i3)
    h_start(i0)
    wo_pass(i0, i2)
    dy_step(i3, i0)
    h_start(i1)
    dy_step(i3, i1)
    h_start(i2)
    dy_take()
    dh_part(i1)
    dh_part(i0)
    finish_dh(i0)
    finish_dh(i2)
    h_pass(i0, i0)
    h_pass(i0, i1)
    h_pass(i2, i1)
    finish_ab(i3)
    dx_part(i0, i0)
    finish_dh(i1)
    dx_part(i0, i1)
    dx_part(i1, i0)
    finish_dh(i3)
    h_pass(i1, i0)
    dx_part(i2, i0)
    relay_db(i0)
    dx_part(i0, i2)
    h_pass(i2, i0)
    dx_part(i2, i1)
    dx_part(i0, i3)
    dx_part(i3, i0)
    h_pass(i0, i2)
    h_pass(i1, i1)
    relay_db(i2)
    dx_part(i2, i2)
    dx_step(i0, i2)
    dx_part(i2, i3)
    h_start(i3)
    dx_part(i1, i1)
    dx_step(i0, i1)
    dx_step(i1, i2)
    relay_db(i1)
    dx_part(i1, i2)
    h_pass(i2, i2)
    dx_part(i1, i3)
    dx_step(i1, i1)
    dx_step(i4, i2)
    dx_step(i4, i1)
    dx_part(i3, i1)
    h_pass(i1, i2)
    relay_db(i3)
    dx_part(i3, i2)
    dx_step(i0, i0)
    dx_step(i5, i2)
    dx_spread(i0)
    h_pass(i3, i0)
    dx_part(i3, i3)
    h_pass(i3, i1)
    out_early()
    dx_step(i4, i0)
    dx_step(i5, i1)
    h_last(i1)
    dx_spread(i4)
    dx_step(i2, i2)
    dx_step(i1, i0)
    h_last(i0)
    dx_step(i5, i0)
    dx_step(i3, i2)
    dx_spread(i1)
    dx_step(i2, i1)
    h_take(i1)
    dx_half(i3)
    dx_step(i3, i1)
    h_last(i2)
    dx_step(i2, i0)
    dx_spread(i2)
    h_pass(i3, i2)
    dx_spread(i5)
    dx_step(i3, i0)
    dx_spread(i3)
    h_take(i2)
    h_take(i0)
    dx_quarter(i3)
    dx_take(i0)
    h_last(i3)
    dx_take(i2)
    dx_take(i1)
    dx_take(i3)
    h_take(i3)

    out(DXR, dxo, "dxo")
    for cond, cp in pending:
        if cond is None:
            cp.wait_send()
        else:
            pl.when(cond)(cp.wait_send)
    for cp in outs:
        cp.wait()


def dw_kernel(x_hbm, dy_hbm, db_hbm, h_hbm, dx_hbm, dwg, dwu, dwo, dxo, XT, DY, DB, H, OA, OB, in_sem, out_sem):
    fq = H.shape[-1]
    loads = [pltpu.make_async_copy(x_hbm, XT, in_sem.at[0])]
    loads += [pltpu.make_async_copy(db_hbm.at[q], DB.at[q], in_sem.at[1 + q]) for q in range(4)]
    loads += [pltpu.make_async_copy(dy_hbm, DY, in_sem.at[5])]
    loads += [pltpu.make_async_copy(h_hbm.at[q], H.at[q], in_sem.at[6 + q]) for q in range(4)]
    for cp in loads:
        cp.start()
    outs = []

    def put(src, dst):
        cp = pltpu.make_async_copy(src, dst, out_sem.at[len(outs)])
        cp.start()
        outs.append(cp)

    loads[0].wait()
    for q in range(4):
        loads[1 + q].wait()
        OA[q] = jnp.dot(XT[...], DB[q], preferred_element_type=F32)
        for m, dst in enumerate((dwg, dwu)):
            put(OA.at[q, :, pl.ds(m * fq, fq)], dst.at[:, pl.ds(q * fq, fq)])
    loads[5].wait()
    for q in range(4):
        loads[6 + q].wait()
        OB[q] = lax.dot_general(H[q], DY[...], TN_DIMS, preferred_element_type=F32)
        put(OB.at[q], dwo.at[pl.ds(q * fq, fq)])
    dxo[...] = dx_hbm[...]
    for cp in outs:
        cp.wait()


def solution(mesh):
    act_spec = P(("dp", "row"), "col")
    weight_spec = P("row", "col")

    def block_backward(x_blk, gy_blk, gate_blk, up_blk, out_blk):
        rows, dm = x_blk.shape
        ff = gate_blk.shape[1]
        fq, tok = ff // 4, 4 * rows
        vm = pltpu.VMEM
        xg, dyg, dbg, hg, dxg = pl.pallas_call(
            lambda *refs: comm_kernel(rows, dm, ff, *refs),
            out_shape=[
                jax.ShapeDtypeStruct((dm, tok), BF16),
                jax.ShapeDtypeStruct((2, 2, rows, dm), BF16),
                jax.ShapeDtypeStruct((4, 4, rows, 2 * fq), BF16),
                jax.ShapeDtypeStruct((2, 2, 4, rows, fq), BF16),
                jax.ShapeDtypeStruct((rows, dm), BF16),
            ],
            in_specs=[ANY] * 5,
            out_specs=[ANY] * 5,
            scratch_shapes=[
                vm((2, 2, 2, rows, dm), BF16),
                vm((2, rows, dm), BF16),
                vm((4, 2, 2, rows, dm), BF16),
                vm((4, dm, 2 * fq), BF16),
                vm((2, dm, 2 * fq), BF16),
                vm((fq, 4 * dm), BF16),
                vm((2, fq, dm // 2), BF16),
                vm((4, rows, 2 * fq), F32),
                vm((4, rows, 2 * fq), F32),
                vm((4, max(RBS), 2 * fq), F32),
                vm((4, rows, fq), F32),
                vm((4, 4, rows, 2 * fq), BF16),
                vm((3, 2, 4, rows, fq), BF16),
                vm((2, 4, rows, fq), BF16),
                vm((2, 2, rows, dm), F32),
                vm((2, 2, rows, dm), F32),
                vm((2, 2, rows, dm), F32),
                vm((2, 2, rows, dm), BF16),
                vm((rows, dm), BF16),
                vm((dm, tok), BF16),
                pltpu.SemaphoreType.DMA((N_SEND,)),
                pltpu.SemaphoreType.DMA((N_RECV,)),
                pltpu.SemaphoreType.DMA((N_LOCAL,)),
            ],
            compiler_params=pltpu.CompilerParams(collective_id=0, has_side_effects=True, vmem_limit_bytes=63 * 1024 * 1024),
            name="comm",
        )(x_blk, gy_blk, gate_blk, up_blk, out_blk)
        whole = pl.BlockSpec(memory_space=vm)
        dw_gate, dw_up, dw_out, grad_x = pl.pallas_call(
            dw_kernel,
            out_shape=[
                jax.ShapeDtypeStruct((dm, ff), F32),
                jax.ShapeDtypeStruct((dm, ff), F32),
                jax.ShapeDtypeStruct((ff, dm), F32),
                jax.ShapeDtypeStruct((rows, dm), BF16),
            ],
            in_specs=[ANY] * 4 + [whole],
            out_specs=[ANY] * 3 + [whole],
            scratch_shapes=[
                vm((dm, tok), BF16), vm((tok, dm), BF16),
                vm((4, tok, 2 * fq), BF16), vm((4, tok, fq), BF16),
                vm((4, dm, 2 * fq), F32), vm((4, fq, dm), F32),
                pltpu.SemaphoreType.DMA((10,)), pltpu.SemaphoreType.DMA((12,)),
            ],
            compiler_params=pltpu.CompilerParams(vmem_limit_bytes=60 * 1024 * 1024),
            name="dw",
        )(xg, dyg.reshape(tok, dm), dbg.reshape(4, tok, 2 * fq), hg.reshape(4, tok, fq), dxg)
        return grad_x, dw_gate, dw_up, dw_out

    return jax.shard_map(block_backward, mesh=mesh, in_specs=(act_spec, act_spec, weight_spec, weight_spec, weight_spec), out_specs=(act_spec, act_spec, act_spec, act_spec), check_vma=False)
```

```python
import math
import jax
import jax.numpy as jnp
from jax import lax
from jax.experimental import pallas as pl
from jax.experimental.pallas import tpu as pltpu
from jax.sharding import PartitionSpec as P

GELU_SCALE = math.sqrt(2.0 / math.pi)
F32, BF16 = jnp.float32, jnp.bfloat16
MESH = pl.DeviceIdType.MESH
ANY = pl.BlockSpec(memory_space=pl.ANY)
NT_DIMS = (((1,), (1,)), ((), ()))
TN_DIMS = (((0,), (0,)), ((), ()))
RBS = (32, 32, 32, 32)
NCH = len(RBS)
CHAIN = 3
OFF = tuple(sum(RBS[:t]) for t in range(NCH))
PIECES = tuple((t, OFF[t] + h * n, n) for t in range(CHAIN) for n in (RBS[t] // (2 if RBS[t] % 32 == 0 else 1),) for h in range(RBS[t] // n))
X_CUT = ((0, 64), (64, 64))
N_CUT = ((0, 256), (256, 384))
NS = range(len(N_CUT))
N_SEND, N_RECV, N_LOCAL = 240, 240, 64


def gelu_pair(pre_f32):
    inner_arg = GELU_SCALE * (pre_f32 + 0.044715 * pre_f32 * pre_f32 * pre_f32)
    tanh_val = jnp.tanh(inner_arg)
    gelu_val = 0.5 * pre_f32 * (1.0 + tanh_val)
    gelu_der = 0.5 * (1.0 + tanh_val) + 0.5 * pre_f32 * (1.0 - tanh_val * tanh_val) * GELU_SCALE * (1.0 + 3.0 * 0.044715 * pre_f32 * pre_f32)
    return gelu_val, gelu_der


class Slots:
    def __init__(self, ref, size):
        self.ref, self.size, self.names, self.used = ref, size, {}, 0

    def __call__(self, *name, off=None):
        if name not in self.names:
            self.names[name] = self.used
            self.used += 1 if off is None else 4
            assert self.used <= self.size
        i = self.names[name]
        return self.ref.at[i if off is None else i + off]


def comm_kernel(rows, dm, ff,
                x_hbm, gy_hbm, wg_hbm, wu_hbm, wo_hbm,
                xo, dyo, dbo, ho, dxo,
                XG, XR, DY, WV, WP, WO, WR, AS, AR, AO, DO, DB, HL, HP, DXS, DXA, DXM, DXF, DXR, XT,
                send_ref, recv_ref, local_ref):
    fq = ff // 4
    cm = dm
    S, R, L = Slots(send_ref, N_SEND), Slots(recv_ref, N_RECV), Slots(local_ref, N_LOCAL)
    p, z, r = lax.axis_index("dp"), lax.axis_index("col"), lax.axis_index("row")
    y, k = r // 2, r % 2
    pr, c = z // 2, z % 2
    zm, zt = z + 1 - 2 * c, z + 2 - 4 * pr
    home, away = y == pr, y != pr
    zeta = jnp.where(y == 0, z, 3 - z)
    zf, zb = z + 1 - 2 * y, z - 1 + 2 * y
    z2 = jnp.where(y == 0, 2, 1)
    jA, jB = y, 1 - y
    ro, rp = 2 * (1 - y) + k, 2 * y + 1 - k
    rx = 2 * (1 - y) + 1 - k
    diag = z == r

    def both(a, b):
        return jnp.logical_and(a, b)

    def dev(z_=z, r_=r, p_=p):
        return {"dp": p_, "col": z_, "row": r_}

    pending = []

    def remote(src, dst, name, to, off=None):
        return pltpu.make_async_remote_copy(src_ref=src, dst_ref=dst, send_sem=S(*name), recv_sem=R(*name, off=off), device_id=to, device_id_type=MESH)

    def send(src, dst, name, to, cond=None, last=None, off=None):
        cp = remote(src, dst, name, to, off)
        if cond is None:
            cp.start()
        else:
            pl.when(cond)(cp.start)
        if last is not False:
            pending.append((cond if last is None else None if last is True else last, cp))

    def got(dst, name, cond=None, off=None):
        cp = remote(dst, dst, name, dev(p_=1 - p), off)
        if cond is None:
            cp.wait_recv()
        else:
            pl.when(cond)(cp.wait_recv)

    def local(src, dst, *name):
        return pltpu.make_async_copy(src, dst, L(*name))

    barrier = pltpu.get_barrier_semaphore()
    peers = [dev(p_=1 - p)] + [dev(z_=(z + dz) % 4, r_=(r + dr) % 4) for dz in range(4) for dr in range(4) if dz or dr]
    for peer in peers:
        pl.semaphore_signal(barrier, inc=1, device_id=peer, device_id_type=MESH)

    lx = local(x_hbm, XG.at[c, k, y], "x")
    pl.when(home)(lx.start)
    ldy = local(gy_hbm, DY.at[z, k, y], "dy")
    ldy.start()
    lw = []
    for m, w in enumerate((wg_hbm, wu_hbm)):
        for q in range(4):
            cp = local(w.at[:, pl.ds(q * fq, fq)], WV.at[q, :, pl.ds(m * fq, fq)], "w", m, q)
            cp.start()
            lw.append(cp)

    half = cm // 2
    pcols = pl.ds(pl.multiple_of(p * half, 512), half)
    line = (z, zm, zt, zt + 1 - 2 * (zt % 2))

    def wo_cut(q, n, cols):
        off, ln = N_CUT[n]
        return wo_hbm.at[pl.ds(pl.multiple_of(q * fq + off, 128), ln), cols]

    def wo_slot(n, src_z, start, width):
        off, ln = N_CUT[n]
        return WO.at[pl.ds(off, ln), pl.ds(pl.multiple_of(src_z * cm + start, 512), width)]

    lwo = []
    for n in NS:
        cp = local(wo_cut(r, n, pl.ds(0, cm)), wo_slot(n, z, 0, cm), "wo", n)
        pl.when(diag)(cp.start)
        lwo.append(cp)
    pl.semaphore_wait(barrier, len(peers))

    def chunk(t):
        return pl.ds(OFF[t], RBS[t])

    def x_place(src_z, ts, cond):
        mine = src_z // 2 == y
        return ((XG.at[src_z % 2, k, y, ts], both(cond, mine)), (XR.at[src_z % 2, ts], both(cond, jnp.logical_not(mine))))

    def x_send(th):
        ts = pl.ds(*X_CUT[th])
        for name, to, cond in (("xr", z + 1, z < 3), ("xl", z - 1, z > 0)):
            for dst, ok in x_place(z, ts, cond):
                send(x_hbm.at[ts], dst, (name, th, 1), dev(z_=to), ok)
        send(x_hbm.at[ts], XG.at[c, k, y, ts], ("xy", th, 0), dev(r_=ro), away)

    def x_step(th, d, left):
        ts = pl.ds(*X_CUT[th])
        src_z, to = (z + d, z - 1) if left else (z - d, z + 1)
        here = src_z <= 3 if left else src_z >= 0
        more = both(here, to >= 0 if left else to <= 3)
        name = "xl" if left else "xr"
        for ref, ok in x_place(src_z, ts, here):
            got(ref, (name, th, d), ok)
            if d < 3:
                send(ref, ref, (name, th, d + 1), dev(z_=to), both(ok, more))
        ref, ok = x_place(src_z, ts, here)[1]
        same = src_z % 2 == c
        send(ref, XG.at[src_z % 2, k, y, ts], ("xy", th, 0), dev(r_=ro), both(ok, same))
        send(ref, XG.at[src_z % 2, k, y, ts], ("xy", th, 1), dev(r_=ro), both(ok, jnp.logical_not(same)))

    def x_give(th):
        ts = pl.ds(*X_CUT[th])
        if th == 0:
            pl.when(home)(lx.wait)
        got(XG.at[c, k, 1 - y, ts], ("xy", th, 0))
        got(XG.at[1 - c, k, 1 - y, ts], ("xy", th, 1))
        send(XG.at[:, k, :, ts], XG.at[:, k, :, ts], ("xd", th), dev(r_=rp))

    def x_take(th):
        got(XG.at[:, 1 - k, :, pl.ds(*X_CUT[th])], ("xd", th))

    def dy_send():
        send(gy_hbm, DY.at[z, k, y], ("dyy",), dev(r_=ro))

    def dy_pass():
        ldy.wait()
        mine = DY.at[z, k]
        got(DY.at[z, k, 1 - y], ("dyy",))
        send(mine, mine, ("dr", 1), dev(z_=z + 1), z < 3)
        send(mine, mine, ("dl", 1), dev(z_=z - 1), z > 0)
        send(mine, mine, ("dyd", 0, 0), dev(r_=rp))

    def dy_from(d, left):
        src_z = z + d if left else z - d
        return src_z, src_z <= 3 if left else src_z >= 0

    def dy_step(d, left):
        src_z, here = dy_from(d, left)
        to = z - 1 if left else z + 1
        more = to >= 0 if left else to <= 3
        name = "dl" if left else "dr"
        theirs = DY.at[src_z, k]
        got(theirs, (name, d), here)
        if d < 3:
            send(theirs, theirs, (name, d + 1), dev(z_=to), both(here, more))
        send(theirs, theirs, ("dyd", d, left), dev(r_=rp), here)

    def dy_take():
        got(DY.at[z, 1 - k], ("dyd", 0, 0))
        for d in range(1, 4):
            for left in range(2):
                src_z, here = dy_from(d, left)
                got(DY.at[src_z, 1 - k], ("dyd", d, left), here)

    def wo_near(n):
        send(wo_cut(rp, n, pl.ds(0, cm)), wo_slot(n, z, 0, cm), ("wn", n), dev(r_=rp), diag)

    def wo_own(n):
        for k2 in range(2):
            q = 2 * y + k2
            send(wo_cut(q, n, pcols), wo_slot(n, z, p * half, half), ("wz", n, k2), dev(z_=r, r_=q), jnp.logical_not(diag), None, z)

    def wo_cross(n):
        off, ln = N_CUT[n]
        for k2 in range(2):
            q = 2 * (1 - y) + k2
            send(wo_cut(q, n, pcols), wo_slot(n, z, p * half, half), ("wd", n, k2), dev(r_=q), diag)
            send(wo_cut(q, n, pcols), WR.at[k2, pl.ds(off, ln)], ("wr", n, k2), dev(r_=ro), jnp.logical_not(diag))

    def wo_relay(n):
        off, ln = N_CUT[n]
        for k2 in range(2):
            got(WR.at[k2, pl.ds(off, ln)], ("wr", n, k2), z != ro)
            send(WR.at[k2, pl.ds(off, ln)], wo_slot(n, z, p * half, half), ("wv", n, k2), dev(z_=ro, r_=2 * y + k2), z != ro, None, z)

    def wo_pass(n, i):
        src_z = line[i]
        mine = wo_slot(n, src_z, p * half, half)
        for k2 in range(2):
            if i == 0:
                got(mine, ("wd", n, k2), both(away, k == k2))
            else:
                got(mine, ("wz", n, k2), both(home, k == k2), src_z)
                got(mine, ("wv", n, k2), both(away, k == k2), src_z)
        send(mine, mine, ("wx", n, i), dev(p_=1 - p), away if i == 0 else None)

    def dh_part(n):
        off, ln = N_CUT[n]
        pl.when(both(home, diag))(lwo[n].wait)
        got(wo_slot(n, z, 0, cm), ("wn", n), both(home, jnp.logical_not(diag)))
        for i in range(4):
            got(wo_slot(n, line[i], (1 - p) * half, half), ("wx", n, i), away if i == 0 else None)

        def go():
            for j in range(4):
                d = lax.dot_general(DY[j].reshape(4 * rows, cm), WO[off:off + ln, j * cm:(j + 1) * cm], NT_DIMS, preferred_element_type=F32).reshape(4, rows, ln)
                DO[:, :, off:off + ln] = d if j == 0 else DO[:, :, off:off + ln] + d

        go()

    def ab_part(s, t):
        tc = 4 * RBS[t]
        own = jnp.dot(XG[k, :, :, OFF[t]:OFF[t] + RBS[t]].reshape(tc, cm), WV[k + 2 * s], preferred_element_type=F32)
        other = jnp.dot(XG[1 - k, :, :, OFF[t]:OFF[t] + RBS[t]].reshape(tc, cm), WP[s], preferred_element_type=F32)
        return (own + other).reshape(4, RBS[t], 2 * fq)

    def ab_mirror(t, cond=None, last=True):
        def go():
            AS[:, OFF[t]:OFF[t] + RBS[t]] = ab_part(1 - y, t)

        go() if cond is None else pl.when(cond)(go)
        send(AS.at[:, chunk(t)], AR.at[:, chunk(t)], ("ab", t), dev(r_=ro), cond, last)

    def weights_here():
        for cp in lw:
            cp.wait()
        for m in range(2):
            for s in range(2):
                got(WP.at[s, :, pl.ds(m * fq, fq)], ("w", m, s))

    hs = jnp.where(home, c, 2)

    def row_blocks(t, fn):
        nb = RBS[t] // 16

        def body(i, _):
            fn(i // nb, pl.ds(pl.multiple_of(OFF[t] + i % nb * 16, 16), 16))
            return 0

        lax.fori_loop(0, 4 * nb, body, 0)

    def finish_ab(t):
        def own():
            AO[:, :RBS[t]] = ab_part(y, t)

        own()
        got(AR.at[:, chunk(t)], ("ab", t))

        def body(o, rs):
            ra = pl.ds(pl.multiple_of(rs.start - OFF[t], 16), 16)
            a = (AO[o, ra, :fq] + AR[o, rs, :fq]).astype(BF16).astype(F32)
            b = (AO[o, ra, fq:] + AR[o, rs, fq:]).astype(BF16).astype(F32)
            g, gd = gelu_pair(a)
            HL[hs, y, o, rs] = (g * b).astype(BF16)
            AR[o, rs, :fq] = b * gd
            AR[o, rs, fq:] = g

        row_blocks(t, body)
        send(HL.at[2, y, :, chunk(t)], HL.at[c, y, :, chunk(t)], ("hy", t), dev(r_=ro), away)

    def finish_dh(t):
        def body(o, rs):
            dh = DO[o, rs]
            DB[r, o, rs, :fq] = (dh * AR[o, rs, :fq]).astype(BF16)
            DB[r, o, rs, fq:] = (dh * AR[o, rs, fq:]).astype(BF16)

        row_blocks(t, body)
        mine = DB.at[r, :, chunk(t)]
        send(mine, mine, ("dby", t), dev(r_=ro))
        send(mine, mine, ("dbd", t), dev(r_=rp))

    def relay_db(t):
        theirs = DB.at[ro, :, chunk(t)]
        got(theirs, ("dby", t))
        send(theirs, theirs, ("dbf", t), dev(r_=rp))

    def h_start(t):
        A, B = HL.at[jA, :, :, chunk(t)], HL.at[jB, :, :, chunk(t)]
        got(HL.at[c, 1 - y, :, chunk(t)], ("hy", t), home)
        send(A, A, ("hA", t), dev(z_=zf), zeta == 0, zeta <= 2)
        send(B, B, ("hB", t), dev(z_=zf), zeta == 1, both(zeta >= 1, zeta <= 2))
        send(B, B, ("hb", t), dev(z_=zb), zeta == 1)

    def h_pass(t, i):
        if i == 0:
            B = HL.at[jB, :, :, chunk(t)]
            got(B, ("hB", t), zeta == 2)
            send(B, B, ("hB", t), dev(z_=zf), zeta == 2, False)
        else:
            A = HL.at[jA, :, :, chunk(t)]
            got(A, ("hA", t), zeta == i)
            send(A, A, ("hA", t), dev(z_=zf), zeta == i, False)

    def h_last(t):
        A, B = HL.at[jA, :, :, chunk(t)], HL.at[jB, :, :, chunk(t)]
        got(B, ("hb", t), zeta == 0)
        got(B, ("hB", t), zeta == 3)
        got(A, ("hA", t), zeta == 3)
        send(HL.at[1 - k, :, :, chunk(t)], HP.at[:, :, chunk(t)], ("hd", t), dev(r_=rp))
        out(HL.at[k, :, :, chunk(t)], ho.at[:, k, :, chunk(t)], "ho", t)

    outs = []

    def out(src, dst, *name):
        cp = local(src, dst, *name)
        cp.start()
        outs.append(cp)

    target = jnp.where(y == 0, k, 1 - k)

    def piece(u):
        return PIECES[u][1:]

    def pieces(t):
        return [u for u in range(len(PIECES)) if PIECES[u][0] == t]

    def dx_part(t, i):
        q = (r, rp, ro, rx)[i]
        theirs = DB.at[q, :, chunk(t)]
        if i == 1:
            got(theirs, ("dbd", t))
        if i == 3:
            got(theirs, ("dbf", t))
            out(DB.at[:, :, chunk(t)], dbo.at[:, :, chunk(t)], "dbo", t)
        sl = slice(OFF[t], OFF[t] + RBS[t])

        def go():
            d = lax.dot_general(DB[q, :, sl].reshape(4 * RBS[t], 2 * fq), WV[q], NT_DIMS, preferred_element_type=F32).reshape(2, 2, RBS[t], cm)
            DXS[:, :, sl] = d if i == 0 else DXS[:, :, sl] + d

        go()
        if i < 3:
            return
        if t < CHAIN:
            for u in pieces(t):
                rs = pl.ds(*piece(u))
                send(DXS.at[:, :, rs], DXA.at[:, :, rs], ("dxa", u), dev(z_=zb), zeta == 3, False)
                send(DXS.at[:, :, rs], DXM.at[:, :, rs], ("dxm", u), dev(z_=zf), both(zeta == 0, target == 1))
        else:
            send(DXS.at[1 - c, :, chunk(t)], DXA.at[0, :, chunk(t)], ("dx1", t), dev(z_=zm))

    def dx_add(u, cond, parts):
        off, ln = piece(u)
        sl = slice(off, off + ln)

        def go():
            for ref in parts:
                DXS[:, :, sl] += ref[:, :, sl]

        pl.when(cond)(go)

    def dx_step(u, at):
        rs = pl.ds(*piece(u))
        on = zeta == at
        goes = both(on, at > target) if at else both(on, target < 0)
        got(DXA.at[:, :, rs], ("dxa", u), both(on, at >= target))
        if at == 1:
            got(DXM.at[:, :, rs], ("dxm", u), both(on, target == 1))
            dx_add(u, both(on, target == 1), (DXA, DXM))
            dx_add(u, both(on, target == 0), (DXA,))
        else:
            dx_add(u, both(on, at >= target), (DXA,))
        if at:
            send(DXS.at[:, :, rs], DXA.at[:, :, rs], ("dxa", u), dev(z_=zb), goes, both(zeta >= 1, zeta > target) if at == 1 else False)

    def dx_spread(u):
        off, ln = piece(u)
        sl, rs = slice(off, off + ln), pl.ds(off, ln)

        @pl.when(diag)
        def _():
            DXF.__setitem__((slice(None), slice(None), sl), DXS[:, :, sl].astype(BF16))

        for k2, y2, i in ((1 - k, y, 0), (k, 1 - y, 1), (1 - k, 1 - y, 2)):
            send(DXF.at[k2, y2, rs], DXR.at[rs], ("dxf", u, i), dev(r_=2 * y2 + k2), diag)

    def dx_half(t):
        sl = slice(OFF[t], OFF[t] + RBS[t])
        got(DXA.at[0, :, chunk(t)], ("dx1", t))

        def go():
            DXS[c, :, sl] += DXA[0, :, sl]

        go()
        send(DXS.at[c, 1 - pr, chunk(t)], DXM.at[0, 0, chunk(t)], ("dx2", t), dev(z_=zt))

    def dx_quarter(t):
        sl = slice(OFF[t], OFF[t] + RBS[t])
        got(DXM.at[0, 0, chunk(t)], ("dx2", t))

        def go():
            DXF[k, y, sl] = (DXS[c, pr, sl] + DXM[0, 0, sl]).astype(BF16)

        go()
        send(DXF.at[k, y, chunk(t)], DXR.at[chunk(t)], ("dxt", t), dev(z_=r, r_=z), jnp.logical_not(diag))

    def w_swap():
        for m, w in enumerate((wg_hbm, wu_hbm)):
            for s in range(2):
                send(w.at[:, pl.ds(pl.multiple_of((1 - k + 2 * s) * fq, 128), fq)], WP.at[s, :, pl.ds(m * fq, fq)], ("w", m, s), dev(r_=rp))

    def h_take(t):
        got(HP.at[:, :, chunk(t)], ("hd", t))
        out(HP.at[:, :, chunk(t)], ho.at[:, 1 - k, :, chunk(t)], "hp", t)

    def dx_take(t):
        sl = slice(OFF[t], OFF[t] + RBS[t])
        zk, zy = z % 2, z // 2

        @pl.when(diag)
        def _():
            DXR.__setitem__(sl, DXF[k, y, sl])

        if t < CHAIN:
            for u in pieces(t):
                rs = pl.ds(*piece(u))
                got(DXR.at[rs], ("dxf", u, 0), both(zk != k, zy == y))
                got(DXR.at[rs], ("dxf", u, 1), both(zk == k, zy != y))
                got(DXR.at[rs], ("dxf", u, 2), both(zk != k, zy != y))
        else:
            got(DXR.at[chunk(t)], ("dxt", t), jnp.logical_not(diag))

    def out_early():
        XT.__setitem__(Ellipsis, XG[k].reshape(4 * rows, cm).T)
        out(XT, xo, "xo")
        out(DY.at[z], dyo, "dyo")

    i0, i1, i2, i3, i4, i5, i6, i7, i8, i9 = range(10)
    yes, no = True, False
    x_send(i0)
    dy_send()
    w_swap()
    wo_cross(i1)
    x_send(i1)
    x_step(i0, i1, i0)
    x_step(i0, i1, i1)
    x_step(i0, i2, i1)
    x_step(i1, i1, i1)
    wo_near(i1)
    x_step(i0, i2, i0)
    x_step(i1, i1, i0)
    dy_pass()
    x_step(i0, i3, i0)
    wo_cross(i0)
    x_step(i1, i2, i0)
    x_step(i0, i3, i1)
    x_step(i1, i3, i0)
    x_step(i1, i2, i1)
    wo_near(i0)
    weights_here()
    wo_relay(i1)
    wo_own(i1)
    x_give(i0)
    dy_step(i1, i0)
    x_step(i1, i3, i1)
    x_take(i0)
    ab_mirror(i0, home, yes)
    dy_step(i1, i1)
    ab_mirror(i1)
    wo_pass(i1, i0)
    x_give(i1)
    wo_own(i0)
    ab_mirror(i0, away, no)
    wo_pass(i0, i0)
    x_take(i1)
    ab_mirror(i2)
    wo_pass(i1, i2)
    wo_pass(i1, i3)
    wo_relay(i0)
    wo_pass(i1, i1)
    finish_ab(i0)
    finish_ab(i1)
    dy_step(i2, i1)
    ab_mirror(i3)
    dy_step(i2, i0)
    wo_pass(i0, i1)
    wo_pass(i0, i3)
    wo_pass(i0, i2)
    dy_step(i3, i0)
    finish_ab(i2)
    h_start(i0)
    dy_step(i3, i1)
    h_start(i1)
    dy_take()
    dh_part(i1)
    dh_part(i0)
    h_pass(i0, i0)
    finish_dh(i0)
    h_pass(i0, i1)
    finish_ab(i3)
    finish_dh(i2)
    dx_part(i2, i0)
    finish_dh(i1)
    dx_part(i0, i0)
    finish_dh(i3)
    dx_part(i3, i0)
    dx_part(i1, i0)
    h_start(i2)
    h_pass(i1, i0)
    dx_part(i0, i1)
    relay_db(i0)
    h_start(i3)
    dx_part(i0, i2)
    dx_part(i0, i3)
    h_pass(i0, i2)
    h_pass(i2, i1)
    dx_part(i2, i1)
    dx_part(i3, i1)
    relay_db(i2)
    dx_part(i2, i2)
    dx_part(i1, i1)
    dx_part(i2, i3)
    h_pass(i2, i0)
    h_last(i0)
    dx_step(i0, i2)
    dx_step(i1, i2)
    relay_db(i1)
    h_pass(i3, i0)
    dx_step(i1, i1)
    dx_part(i1, i2)
    dx_part(i1, i3)
    dx_step(i0, i1)
    h_pass(i1, i1)
    dx_step(i4, i2)
    h_pass(i3, i1)
    relay_db(i3)
    h_pass(i2, i2)
    dx_step(i4, i1)
    dx_step(i5, i2)
    dx_part(i3, i2)
    dx_step(i1, i0)
    dx_step(i4, i0)
    dx_part(i3, i3)
    dx_step(i5, i1)
    dx_spread(i4)
    dx_step(i2, i2)
    dx_spread(i1)
    h_pass(i1, i2)
    dx_step(i5, i0)
    out_early()
    h_take(i0)
    dx_step(i3, i2)
    dx_step(i2, i1)
    dx_spread(i5)
    h_last(i1)
    dx_half(i3)
    dx_step(i2, i0)
    h_last(i2)
    dx_spread(i2)
    dx_step(i0, i0)
    dx_spread(i0)
    dx_step(i3, i1)
    h_take(i2)
    dx_step(i3, i0)
    dx_spread(i3)
    h_take(i1)
    dx_take(i2)
    h_pass(i3, i2)
    dx_quarter(i3)
    h_last(i3)
    dx_take(i0)
    dx_take(i1)
    dx_take(i3)
    h_take(i3)

    out(DXR, dxo, "dxo")
    for cond, cp in pending:
        if cond is None:
            cp.wait_send()
        else:
            pl.when(cond)(cp.wait_send)
    for cp in outs:
        cp.wait()


def dw_kernel(x_hbm, dy_hbm, db_hbm, h_hbm, dx_hbm, dwg, dwu, dwo, dxo, XT, DY, DB, H, DX, OA, OB, in_sem, out_sem):
    fq = H.shape[-1]
    loads = [pltpu.make_async_copy(x_hbm, XT, in_sem.at[0])]
    loads += [pltpu.make_async_copy(db_hbm.at[q], DB.at[q], in_sem.at[1 + q]) for q in range(4)]
    loads += [pltpu.make_async_copy(dy_hbm, DY, in_sem.at[5])]
    loads += [pltpu.make_async_copy(h_hbm.at[q], H.at[q], in_sem.at[6 + q]) for q in range(4)]
    loads += [pltpu.make_async_copy(dx_hbm, DX, in_sem.at[10])]
    for cp in loads:
        cp.start()
    outs = []

    def put(src, dst):
        cp = pltpu.make_async_copy(src, dst, out_sem.at[len(outs)])
        cp.start()
        outs.append(cp)

    loads[0].wait()
    for q in range(4):
        loads[1 + q].wait()
        OA[q] = jnp.dot(XT[...], DB[q], preferred_element_type=F32)
        for m, dst in enumerate((dwg, dwu)):
            put(OA.at[q, :, pl.ds(m * fq, fq)], dst.at[:, pl.ds(q * fq, fq)])
    loads[10].wait()
    put(DX, dxo)
    loads[5].wait()
    for q in range(4):
        loads[6 + q].wait()
        OB[q] = lax.dot_general(H[q], DY[...], TN_DIMS, preferred_element_type=F32)
        put(OB.at[q], dwo.at[pl.ds(q * fq, fq)])
    for cp in outs:
        cp.wait()


def solution(mesh):
    act_spec = P(("dp", "row"), "col")
    weight_spec = P("row", "col")

    def block_backward(x_blk, gy_blk, gate_blk, up_blk, out_blk):
        rows, dm = x_blk.shape
        ff = gate_blk.shape[1]
        fq, tok = ff // 4, 4 * rows
        vm = pltpu.VMEM
        xg, dyg, dbg, hg, dxg = pl.pallas_call(
            lambda *refs: comm_kernel(rows, dm, ff, *refs),
            out_shape=[
                jax.ShapeDtypeStruct((dm, tok), BF16),
                jax.ShapeDtypeStruct((2, 2, rows, dm), BF16),
                jax.ShapeDtypeStruct((4, 4, rows, 2 * fq), BF16),
                jax.ShapeDtypeStruct((2, 2, 4, rows, fq), BF16),
                jax.ShapeDtypeStruct((rows, dm), BF16),
            ],
            in_specs=[ANY] * 5,
            out_specs=[ANY] * 5,
            scratch_shapes=[
                vm((2, 2, 2, rows, dm), BF16),
                vm((2, rows, dm), BF16),
                vm((4, 2, 2, rows, dm), BF16),
                vm((4, dm, 2 * fq), BF16),
                vm((2, dm, 2 * fq), BF16),
                vm((fq, 4 * dm), BF16),
                vm((2, fq, dm // 2), BF16),
                vm((4, rows, 2 * fq), F32),
                vm((4, rows, 2 * fq), F32),
                vm((4, max(RBS), 2 * fq), F32),
                vm((4, rows, fq), F32),
                vm((4, 4, rows, 2 * fq), BF16),
                vm((3, 2, 4, rows, fq), BF16),
                vm((2, 4, rows, fq), BF16),
                vm((2, 2, rows, dm), F32),
                vm((2, 2, rows, dm), F32),
                vm((2, 2, rows, dm), F32),
                vm((2, 2, rows, dm), BF16),
                vm((rows, dm), BF16),
                vm((dm, tok), BF16),
                pltpu.SemaphoreType.DMA((N_SEND,)),
                pltpu.SemaphoreType.DMA((N_RECV,)),
                pltpu.SemaphoreType.DMA((N_LOCAL,)),
            ],
            compiler_params=pltpu.CompilerParams(collective_id=0, has_side_effects=True, vmem_limit_bytes=63 * 1024 * 1024),
            name="comm",
        )(x_blk, gy_blk, gate_blk, up_blk, out_blk)
        dw_gate, dw_up, dw_out, grad_x = pl.pallas_call(
            dw_kernel,
            out_shape=[
                jax.ShapeDtypeStruct((dm, ff), F32),
                jax.ShapeDtypeStruct((dm, ff), F32),
                jax.ShapeDtypeStruct((ff, dm), F32),
                jax.ShapeDtypeStruct((rows, dm), BF16),
            ],
            in_specs=[ANY] * 5,
            out_specs=[ANY] * 4,
            scratch_shapes=[
                vm((dm, tok), BF16), vm((tok, dm), BF16),
                vm((4, tok, 2 * fq), BF16), vm((4, tok, fq), BF16), vm((rows, dm), BF16),
                vm((4, dm, 2 * fq), F32), vm((4, fq, dm), F32),
                pltpu.SemaphoreType.DMA((11,)), pltpu.SemaphoreType.DMA((13,)),
            ],
            compiler_params=pltpu.CompilerParams(vmem_limit_bytes=60 * 1024 * 1024),
            name="dw",
        )(xg, dyg.reshape(tok, dm), dbg.reshape(4, tok, 2 * fq), hg.reshape(4, tok, fq), dxg)
        return grad_x, dw_gate, dw_up, dw_out

    return jax.shard_map(block_backward, mesh=mesh, in_specs=(act_spec, act_spec, weight_spec, weight_spec, weight_spec), out_specs=(act_spec, act_spec, act_spec, act_spec), check_vma=False)
```

```python
import math
import jax
import jax.numpy as jnp
from jax import lax
from jax.experimental import pallas as pl
from jax.experimental.pallas import tpu as pltpu
from jax.sharding import PartitionSpec as P

GELU_SCALE = math.sqrt(2.0 / math.pi)
F32, BF16 = jnp.float32, jnp.bfloat16
MESH = pl.DeviceIdType.MESH
ANY = pl.BlockSpec(memory_space=pl.ANY)
NT_DIMS = (((1,), (1,)), ((), ()))
TN_DIMS = (((0,), (0,)), ((), ()))
RBS = (32, 32, 32, 32)
NCH = len(RBS)
CHAIN = 3
OFF = tuple(sum(RBS[:t]) for t in range(NCH))
PIECES = tuple((t, OFF[t] + h * n, n) for t in range(CHAIN) for n in (RBS[t] // (2 if RBS[t] % 32 == 0 else 1),) for h in range(RBS[t] // n))
X_CUT = ((0, 64), (64, 64))
N_CUT = ((0, 256), (256, 384))
NS = range(len(N_CUT))
N_SEND, N_RECV, N_LOCAL = 240, 240, 64


def gelu_pair(pre_f32):
    inner_arg = GELU_SCALE * (pre_f32 + 0.044715 * pre_f32 * pre_f32 * pre_f32)
    tanh_val = jnp.tanh(inner_arg)
    gelu_val = 0.5 * pre_f32 * (1.0 + tanh_val)
    gelu_der = 0.5 * (1.0 + tanh_val) + 0.5 * pre_f32 * (1.0 - tanh_val * tanh_val) * GELU_SCALE * (1.0 + 3.0 * 0.044715 * pre_f32 * pre_f32)
    return gelu_val, gelu_der


class Slots:
    def __init__(self, ref, size):
        self.ref, self.size, self.names, self.used = ref, size, {}, 0

    def __call__(self, *name, off=None):
        if name not in self.names:
            self.names[name] = self.used
            self.used += 1 if off is None else 4
            assert self.used <= self.size
        i = self.names[name]
        return self.ref.at[i if off is None else i + off]


def comm_kernel(rows, dm, ff,
                x_hbm, gy_hbm, wg_hbm, wu_hbm, wo_hbm,
                xo, dyo, dbo, ho, dxo,
                XG, XR, DY, WV, WP, WO, WR, AS, AR, AO, DO, DB, HL, HP, DXS, DXA, DXM, DXF, DXR, XT,
                send_ref, recv_ref, local_ref):
    fq = ff // 4
    cm = dm
    S, R, L = Slots(send_ref, N_SEND), Slots(recv_ref, N_RECV), Slots(local_ref, N_LOCAL)
    p, z, r = lax.axis_index("dp"), lax.axis_index("col"), lax.axis_index("row")
    y, k = r // 2, r % 2
    pr, c = z // 2, z % 2
    zm, zt = z + 1 - 2 * c, z + 2 - 4 * pr
    home, away = y == pr, y != pr
    zeta = jnp.where(y == 0, z, 3 - z)
    zf, zb = z + 1 - 2 * y, z - 1 + 2 * y
    z2 = jnp.where(y == 0, 2, 1)
    jA, jB = y, 1 - y
    ro, rp = 2 * (1 - y) + k, 2 * y + 1 - k
    rx = 2 * (1 - y) + 1 - k
    diag = z == r

    def both(a, b):
        return jnp.logical_and(a, b)

    def dev(z_=z, r_=r, p_=p):
        return {"dp": p_, "col": z_, "row": r_}

    pending = []

    def remote(src, dst, name, to, off=None):
        return pltpu.make_async_remote_copy(src_ref=src, dst_ref=dst, send_sem=S(*name), recv_sem=R(*name, off=off), device_id=to, device_id_type=MESH)

    def send(src, dst, name, to, cond=None, last=None, off=None):
        cp = remote(src, dst, name, to, off)
        if cond is None:
            cp.start()
        else:
            pl.when(cond)(cp.start)
        if last is not False:
            pending.append((cond if last is None else None if last is True else last, cp))

    def got(dst, name, cond=None, off=None):
        cp = remote(dst, dst, name, dev(p_=1 - p), off)
        if cond is None:
            cp.wait_recv()
        else:
            pl.when(cond)(cp.wait_recv)

    def local(src, dst, *name):
        return pltpu.make_async_copy(src, dst, L(*name))

    barrier = pltpu.get_barrier_semaphore()
    peers = [dev(p_=1 - p), dev(r_=ro), dev(r_=rx)]
    peers += [dev(z_=(z + dz) % 4, r_=2 * y + (k + dk) % 2) for dz in range(4) for dk in range(2) if dz or dk]
    for peer in peers:
        pl.semaphore_signal(barrier, inc=1, device_id=peer, device_id_type=MESH)

    @pl.when(jnp.logical_not(diag))
    def _():
        pl.semaphore_signal(barrier, inc=1, device_id=dev(z_=r, r_=z), device_id_type=MESH)

    lx = local(x_hbm, XG.at[c, k, y], "x")
    pl.when(home)(lx.start)
    ldy = local(gy_hbm, DY.at[z, k, y], "dy")
    ldy.start()
    lw = []
    for m, w in enumerate((wg_hbm, wu_hbm)):
        for q in range(4):
            cp = local(w.at[:, pl.ds(q * fq, fq)], WV.at[q, :, pl.ds(m * fq, fq)], "w", m, q)
            cp.start()
            lw.append(cp)

    half = cm // 2
    pcols = pl.ds(pl.multiple_of(p * half, 512), half)
    line = (z, zm, zt, zt + 1 - 2 * (zt % 2))

    def wo_cut(q, n, cols):
        off, ln = N_CUT[n]
        return wo_hbm.at[pl.ds(pl.multiple_of(q * fq + off, 128), ln), cols]

    def wo_slot(n, src_z, start, width):
        off, ln = N_CUT[n]
        return WO.at[pl.ds(off, ln), pl.ds(pl.multiple_of(src_z * cm + start, 512), width)]

    lwo = []
    for n in NS:
        cp = local(wo_cut(r, n, pl.ds(0, cm)), wo_slot(n, z, 0, cm), "wo", n)
        pl.when(diag)(cp.start)
        lwo.append(cp)
    pl.semaphore_wait(barrier, jnp.where(diag, len(peers), len(peers) + 1))

    def chunk(t):
        return pl.ds(OFF[t], RBS[t])

    def x_place(src_z, ts, cond):
        mine = src_z // 2 == y
        return ((XG.at[src_z % 2, k, y, ts], both(cond, mine)), (XR.at[src_z % 2, ts], both(cond, jnp.logical_not(mine))))

    def x_send(th):
        ts = pl.ds(*X_CUT[th])
        for name, to, cond in (("xr", z + 1, z < 3), ("xl", z - 1, z > 0)):
            for dst, ok in x_place(z, ts, cond):
                send(x_hbm.at[ts], dst, (name, th, 1), dev(z_=to), ok)
        send(x_hbm.at[ts], XG.at[c, k, y, ts], ("xy", th, 0), dev(r_=ro), away)

    def x_step(th, d, left):
        ts = pl.ds(*X_CUT[th])
        src_z, to = (z + d, z - 1) if left else (z - d, z + 1)
        here = src_z <= 3 if left else src_z >= 0
        more = both(here, to >= 0 if left else to <= 3)
        name = "xl" if left else "xr"
        for ref, ok in x_place(src_z, ts, here):
            got(ref, (name, th, d), ok)
            if d < 3:
                send(ref, ref, (name, th, d + 1), dev(z_=to), both(ok, more))
        ref, ok = x_place(src_z, ts, here)[1]
        same = src_z % 2 == c
        send(ref, XG.at[src_z % 2, k, y, ts], ("xy", th, 0), dev(r_=ro), both(ok, same))
        send(ref, XG.at[src_z % 2, k, y, ts], ("xy", th, 1), dev(r_=ro), both(ok, jnp.logical_not(same)))

    def x_give(th):
        ts = pl.ds(*X_CUT[th])
        if th == 0:
            pl.when(home)(lx.wait)
        got(XG.at[c, k, 1 - y, ts], ("xy", th, 0))
        got(XG.at[1 - c, k, 1 - y, ts], ("xy", th, 1))
        send(XG.at[:, k, :, ts], XG.at[:, k, :, ts], ("xd", th), dev(r_=rp))

    def x_take(th):
        got(XG.at[:, 1 - k, :, pl.ds(*X_CUT[th])], ("xd", th))

    def dy_send():
        send(gy_hbm, DY.at[z, k, y], ("dyy",), dev(r_=ro))

    def dy_pass():
        ldy.wait()
        mine = DY.at[z, k]
        got(DY.at[z, k, 1 - y], ("dyy",))
        send(mine, mine, ("dr", 1), dev(z_=z + 1), z < 3)
        send(mine, mine, ("dl", 1), dev(z_=z - 1), z > 0)
        send(mine, mine, ("dyd", 0, 0), dev(r_=rp))

    def dy_from(d, left):
        src_z = z + d if left else z - d
        return src_z, src_z <= 3 if left else src_z >= 0

    def dy_step(d, left):
        src_z, here = dy_from(d, left)
        to = z - 1 if left else z + 1
        more = to >= 0 if left else to <= 3
        name = "dl" if left else "dr"
        theirs = DY.at[src_z, k]
        got(theirs, (name, d), here)
        if d < 3:
            send(theirs, theirs, (name, d + 1), dev(z_=to), both(here, more))
        send(theirs, theirs, ("dyd", d, left), dev(r_=rp), here)

    def dy_take():
        got(DY.at[z, 1 - k], ("dyd", 0, 0))
        for d in range(1, 4):
            for left in range(2):
                src_z, here = dy_from(d, left)
                got(DY.at[src_z, 1 - k], ("dyd", d, left), here)

    def wo_near(n):
        send(wo_cut(rp, n, pl.ds(0, cm)), wo_slot(n, z, 0, cm), ("wn", n), dev(r_=rp), diag)

    def wo_own(n):
        for k2 in range(2):
            q = 2 * y + k2
            send(wo_cut(q, n, pcols), wo_slot(n, z, p * half, half), ("wz", n, k2), dev(z_=r, r_=q), jnp.logical_not(diag), None, z)

    def wo_cross(n):
        off, ln = N_CUT[n]
        for k2 in range(2):
            q = 2 * (1 - y) + k2
            send(wo_cut(q, n, pcols), wo_slot(n, z, p * half, half), ("wd", n, k2), dev(r_=q), diag)
            send(wo_cut(q, n, pcols), WR.at[k2, pl.ds(off, ln)], ("wr", n, k2), dev(r_=ro), jnp.logical_not(diag))

    def wo_relay(n):
        off, ln = N_CUT[n]
        for k2 in range(2):
            got(WR.at[k2, pl.ds(off, ln)], ("wr", n, k2), z != ro)
            send(WR.at[k2, pl.ds(off, ln)], wo_slot(n, z, p * half, half), ("wv", n, k2), dev(z_=ro, r_=2 * y + k2), z != ro, None, z)

    def wo_pass(n, i):
        src_z = line[i]
        mine = wo_slot(n, src_z, p * half, half)
        for k2 in range(2):
            if i == 0:
                got(mine, ("wd", n, k2), both(away, k == k2))
            else:
                got(mine, ("wz", n, k2), both(home, k == k2), src_z)
                got(mine, ("wv", n, k2), both(away, k == k2), src_z)
        send(mine, mine, ("wx", n, i), dev(p_=1 - p), away if i == 0 else None)

    def dh_part(n):
        off, ln = N_CUT[n]
        pl.when(both(home, diag))(lwo[n].wait)
        got(wo_slot(n, z, 0, cm), ("wn", n), both(home, jnp.logical_not(diag)))
        for i in range(4):
            got(wo_slot(n, line[i], (1 - p) * half, half), ("wx", n, i), away if i == 0 else None)

        def go():
            for j in range(4):
                d = lax.dot_general(DY[j].reshape(4 * rows, cm), WO[off:off + ln, j * cm:(j + 1) * cm], NT_DIMS, preferred_element_type=F32).reshape(4, rows, ln)
                DO[:, :, off:off + ln] = d if j == 0 else DO[:, :, off:off + ln] + d

        go()

    def ab_part(s, t):
        tc = 4 * RBS[t]
        own = jnp.dot(XG[k, :, :, OFF[t]:OFF[t] + RBS[t]].reshape(tc, cm), WV[k + 2 * s], preferred_element_type=F32)
        other = jnp.dot(XG[1 - k, :, :, OFF[t]:OFF[t] + RBS[t]].reshape(tc, cm), WP[s], preferred_element_type=F32)
        return (own + other).reshape(4, RBS[t], 2 * fq)

    def ab_mirror(t, cond=None, last=True):
        def go():
            AS[:, OFF[t]:OFF[t] + RBS[t]] = ab_part(1 - y, t)

        go() if cond is None else pl.when(cond)(go)
        send(AS.at[:, chunk(t)], AR.at[:, chunk(t)], ("ab", t), dev(r_=ro), cond, last)

    def weights_here():
        for cp in lw:
            cp.wait()
        for m in range(2):
            for s in range(2):
                got(WP.at[s, :, pl.ds(m * fq, fq)], ("w", m, s))

    hs = jnp.where(home, c, 2)

    def row_blocks(t, fn):
        nb = RBS[t] // 16

        def body(i, _):
            fn(i // nb, pl.ds(pl.multiple_of(OFF[t] + i % nb * 16, 16), 16))
            return 0

        lax.fori_loop(0, 4 * nb, body, 0)

    def finish_ab(t):
        def own():
            AO[:, :RBS[t]] = ab_part(y, t)

        own()
        got(AR.at[:, chunk(t)], ("ab", t))

        def body(o, rs):
            ra = pl.ds(pl.multiple_of(rs.start - OFF[t], 16), 16)
            a = (AO[o, ra, :fq] + AR[o, rs, :fq]).astype(BF16).astype(F32)
            b = (AO[o, ra, fq:] + AR[o, rs, fq:]).astype(BF16).astype(F32)
            g, gd = gelu_pair(a)
            HL[hs, y, o, rs] = (g * b).astype(BF16)
            AR[o, rs, :fq] = b * gd
            AR[o, rs, fq:] = g

        row_blocks(t, body)
        send(HL.at[2, y, :, chunk(t)], HL.at[c, y, :, chunk(t)], ("hy", t), dev(r_=ro), away)

    def finish_dh(t):
        def body(o, rs):
            dh = DO[o, rs]
            DB[r, o, rs, :fq] = (dh * AR[o, rs, :fq]).astype(BF16)
            DB[r, o, rs, fq:] = (dh * AR[o, rs, fq:]).astype(BF16)

        row_blocks(t, body)
        mine = DB.at[r, :, chunk(t)]
        send(mine, mine, ("dby", t), dev(r_=ro))
        send(mine, mine, ("dbd", t), dev(r_=rp))

    def relay_db(t):
        theirs = DB.at[ro, :, chunk(t)]
        got(theirs, ("dby", t))
        send(theirs, theirs, ("dbf", t), dev(r_=rp))

    def h_start(t):
        A, B = HL.at[jA, :, :, chunk(t)], HL.at[jB, :, :, chunk(t)]
        got(HL.at[c, 1 - y, :, chunk(t)], ("hy", t), home)
        send(A, A, ("hA", t), dev(z_=zf), zeta == 0, zeta <= 2)
        send(B, B, ("hB", t), dev(z_=zf), zeta == 1, both(zeta >= 1, zeta <= 2))
        send(B, B, ("hb", t), dev(z_=zb), zeta == 1)

    def h_pass(t, i):
        if i == 0:
            B = HL.at[jB, :, :, chunk(t)]
            got(B, ("hB", t), zeta == 2)
            send(B, B, ("hB", t), dev(z_=zf), zeta == 2, False)
        else:
            A = HL.at[jA, :, :, chunk(t)]
            got(A, ("hA", t), zeta == i)
            send(A, A, ("hA", t), dev(z_=zf), zeta == i, False)

    def h_last(t):
        A, B = HL.at[jA, :, :, chunk(t)], HL.at[jB, :, :, chunk(t)]
        got(B, ("hb", t), zeta == 0)
        got(B, ("hB", t), zeta == 3)
        got(A, ("hA", t), zeta == 3)
        send(HL.at[1 - k, :, :, chunk(t)], HP.at[:, :, chunk(t)], ("hd", t), dev(r_=rp))
        out(HL.at[k, :, :, chunk(t)], ho.at[:, k, :, chunk(t)], "ho", t)

    outs = []

    def out(src, dst, *name):
        cp = local(src, dst, *name)
        cp.start()
        outs.append(cp)

    target = jnp.where(y == 0, k, 1 - k)

    def piece(u):
        return PIECES[u][1:]

    def pieces(t):
        return [u for u in range(len(PIECES)) if PIECES[u][0] == t]

    def dx_part(t, i):
        q = (r, rp, ro, rx)[i]
        theirs = DB.at[q, :, chunk(t)]
        if i == 1:
            got(theirs, ("dbd", t))
        if i == 3:
            got(theirs, ("dbf", t))
            out(DB.at[:, :, chunk(t)], dbo.at[:, :, chunk(t)], "dbo", t)
        sl = slice(OFF[t], OFF[t] + RBS[t])

        def go():
            d = lax.dot_general(DB[q, :, sl].reshape(4 * RBS[t], 2 * fq), WV[q], NT_DIMS, preferred_element_type=F32).reshape(2, 2, RBS[t], cm)
            DXS[:, :, sl] = d if i == 0 else DXS[:, :, sl] + d

        go()
        if i < 3:
            return
        if t < CHAIN:
            for u in pieces(t):
                rs = pl.ds(*piece(u))
                send(DXS.at[:, :, rs], DXA.at[:, :, rs], ("dxa", u), dev(z_=zb), zeta == 3, False)
                send(DXS.at[:, :, rs], DXM.at[:, :, rs], ("dxm", u), dev(z_=zf), both(zeta == 0, target == 1))
        else:
            send(DXS.at[1 - c, :, chunk(t)], DXA.at[0, :, chunk(t)], ("dx1", t), dev(z_=zm))

    def dx_add(u, cond, parts):
        off, ln = piece(u)
        sl = slice(off, off + ln)

        def go():
            for ref in parts:
                DXS[:, :, sl] += ref[:, :, sl]

        pl.when(cond)(go)

    def dx_step(u, at):
        rs = pl.ds(*piece(u))
        on = zeta == at
        goes = both(on, at > target) if at else both(on, target < 0)
        got(DXA.at[:, :, rs], ("dxa", u), both(on, at >= target))
        if at == 1:
            got(DXM.at[:, :, rs], ("dxm", u), both(on, target == 1))
            dx_add(u, both(on, target == 1), (DXA, DXM))
            dx_add(u, both(on, target == 0), (DXA,))
        else:
            dx_add(u, both(on, at >= target), (DXA,))
        if at:
            send(DXS.at[:, :, rs], DXA.at[:, :, rs], ("dxa", u), dev(z_=zb), goes, both(zeta >= 1, zeta > target) if at == 1 else False)

    def dx_spread(u):
        off, ln = piece(u)
        sl, rs = slice(off, off + ln), pl.ds(off, ln)

        @pl.when(diag)
        def _():
            DXF.__setitem__((slice(None), slice(None), sl), DXS[:, :, sl].astype(BF16))

        for k2, y2, i in ((1 - k, y, 0), (k, 1 - y, 1), (1 - k, 1 - y, 2)):
            send(DXF.at[k2, y2, rs], DXR.at[rs], ("dxf", u, i), dev(r_=2 * y2 + k2), diag)

    def dx_half(t):
        sl = slice(OFF[t], OFF[t] + RBS[t])
        got(DXA.at[0, :, chunk(t)], ("dx1", t))

        def go():
            DXS[c, :, sl] += DXA[0, :, sl]

        go()
        send(DXS.at[c, 1 - pr, chunk(t)], DXM.at[0, 0, chunk(t)], ("dx2", t), dev(z_=zt))

    def dx_quarter(t):
        sl = slice(OFF[t], OFF[t] + RBS[t])
        got(DXM.at[0, 0, chunk(t)], ("dx2", t))

        def go():
            DXF[k, y, sl] = (DXS[c, pr, sl] + DXM[0, 0, sl]).astype(BF16)

        go()
        send(DXF.at[k, y, chunk(t)], DXR.at[chunk(t)], ("dxt", t), dev(z_=r, r_=z), jnp.logical_not(diag))

    def w_swap():
        for m, w in enumerate((wg_hbm, wu_hbm)):
            for s in range(2):
                send(w.at[:, pl.ds(pl.multiple_of((1 - k + 2 * s) * fq, 128), fq)], WP.at[s, :, pl.ds(m * fq, fq)], ("w", m, s), dev(r_=rp))

    def h_take(t):
        got(HP.at[:, :, chunk(t)], ("hd", t))
        out(HP.at[:, :, chunk(t)], ho.at[:, 1 - k, :, chunk(t)], "hp", t)

    def dx_take(t):
        sl = slice(OFF[t], OFF[t] + RBS[t])
        zk, zy = z % 2, z // 2

        @pl.when(diag)
        def _():
            DXR.__setitem__(sl, DXF[k, y, sl])

        if t < CHAIN:
            for u in pieces(t):
                rs = pl.ds(*piece(u))
                got(DXR.at[rs], ("dxf", u, 0), both(zk != k, zy == y))
                got(DXR.at[rs], ("dxf", u, 1), both(zk == k, zy != y))
                got(DXR.at[rs], ("dxf", u, 2), both(zk != k, zy != y))
        else:
            got(DXR.at[chunk(t)], ("dxt", t), jnp.logical_not(diag))

    def out_early():
        XT.__setitem__(Ellipsis, XG[k].reshape(4 * rows, cm).T)
        out(XT, xo, "xo")
        out(DY.at[z], dyo, "dyo")

    i0, i1, i2, i3, i4, i5, i6, i7, i8, i9 = range(10)
    yes, no = True, False
    x_send(i0)
    dy_send()
    w_swap()
    wo_cross(i1)
    x_send(i1)
    x_step(i0, i1, i0)
    x_step(i0, i1, i1)
    x_step(i0, i2, i1)
    x_step(i1, i1, i1)
    wo_near(i1)
    x_step(i0, i2, i0)
    x_step(i1, i1, i0)
    dy_pass()
    x_step(i0, i3, i0)
    wo_cross(i0)
    x_step(i1, i2, i0)
    x_step(i0, i3, i1)
    x_step(i1, i3, i0)
    x_step(i1, i2, i1)
    wo_near(i0)
    weights_here()
    wo_relay(i1)
    wo_own(i1)
    x_give(i0)
    dy_step(i1, i0)
    x_step(i1, i3, i1)
    x_take(i0)
    ab_mirror(i0, home, yes)
    dy_step(i1, i1)
    ab_mirror(i1)
    wo_pass(i1, i0)
    x_give(i1)
    wo_own(i0)
    ab_mirror(i0, away, no)
    wo_pass(i0, i0)
    x_take(i1)
    ab_mirror(i2)
    wo_pass(i1, i2)
    wo_pass(i1, i3)
    wo_relay(i0)
    wo_pass(i1, i1)
    finish_ab(i0)
    finish_ab(i1)
    dy_step(i2, i1)
    ab_mirror(i3)
    dy_step(i2, i0)
    wo_pass(i0, i1)
    wo_pass(i0, i3)
    wo_pass(i0, i2)
    dy_step(i3, i0)
    finish_ab(i2)
    h_start(i0)
    dy_step(i3, i1)
    h_start(i1)
    dy_take()
    dh_part(i1)
    dh_part(i0)
    h_pass(i0, i0)
    finish_dh(i0)
    h_pass(i0, i1)
    finish_ab(i3)
    finish_dh(i2)
    dx_part(i2, i0)
    finish_dh(i1)
    dx_part(i0, i0)
    finish_dh(i3)
    dx_part(i3, i0)
    dx_part(i1, i0)
    h_start(i2)
    h_pass(i1, i0)
    dx_part(i0, i1)
    relay_db(i0)
    h_start(i3)
    dx_part(i0, i2)
    dx_part(i0, i3)
    h_pass(i0, i2)
    h_pass(i2, i1)
    dx_part(i2, i1)
    dx_part(i3, i1)
    relay_db(i2)
    dx_part(i2, i2)
    dx_part(i1, i1)
    dx_part(i2, i3)
    h_pass(i2, i0)
    h_last(i0)
    dx_step(i0, i2)
    dx_step(i1, i2)
    relay_db(i1)
    h_pass(i3, i0)
    dx_step(i1, i1)
    dx_part(i1, i2)
    dx_part(i1, i3)
    dx_step(i0, i1)
    h_pass(i1, i1)
    dx_step(i4, i2)
    h_pass(i3, i1)
    relay_db(i3)
    h_pass(i2, i2)
    dx_step(i4, i1)
    dx_step(i5, i2)
    dx_part(i3, i2)
    dx_step(i1, i0)
    dx_step(i4, i0)
    dx_part(i3, i3)
    dx_step(i5, i1)
    dx_spread(i4)
    dx_step(i2, i2)
    dx_spread(i1)
    h_pass(i1, i2)
    dx_step(i5, i0)
    out_early()
    h_take(i0)
    dx_step(i3, i2)
    dx_step(i2, i1)
    dx_spread(i5)
    h_last(i1)
    dx_half(i3)
    dx_step(i2, i0)
    h_last(i2)
    dx_spread(i2)
    dx_step(i0, i0)
    dx_spread(i0)
    dx_step(i3, i1)
    h_take(i2)
    dx_step(i3, i0)
    dx_spread(i3)
    h_take(i1)
    dx_take(i2)
    h_pass(i3, i2)
    dx_quarter(i3)
    h_last(i3)
    dx_take(i0)
    dx_take(i1)
    dx_take(i3)
    h_take(i3)

    out(DXR, dxo, "dxo")
    for cond, cp in pending:
        if cond is None:
            cp.wait_send()
        else:
            pl.when(cond)(cp.wait_send)
    for cp in outs:
        cp.wait()


def dw_kernel(x_hbm, dy_hbm, db_hbm, h_hbm, dx_hbm, dwg, dwu, dwo, dxo, XT, DY, DB, H, DX, OA, OB, in_sem, out_sem):
    fq = H.shape[-1]
    loads = [pltpu.make_async_copy(x_hbm, XT, in_sem.at[0])]
    loads += [pltpu.make_async_copy(db_hbm.at[q], DB.at[q], in_sem.at[1 + q]) for q in range(4)]
    loads += [pltpu.make_async_copy(dy_hbm, DY, in_sem.at[5])]
    loads += [pltpu.make_async_copy(h_hbm.at[q], H.at[q], in_sem.at[6 + q]) for q in range(4)]
    loads += [pltpu.make_async_copy(dx_hbm, DX, in_sem.at[10])]
    for cp in loads:
        cp.start()
    outs = []

    def put(src, dst):
        cp = pltpu.make_async_copy(src, dst, out_sem.at[len(outs)])
        cp.start()
        outs.append(cp)

    loads[0].wait()
    for q in range(4):
        loads[1 + q].wait()
        OA[q] = jnp.dot(XT[...], DB[q], preferred_element_type=F32)
        for m, dst in enumerate((dwg, dwu)):
            put(OA.at[q, :, pl.ds(m * fq, fq)], dst.at[:, pl.ds(q * fq, fq)])
    loads[10].wait()
    put(DX, dxo)
    loads[5].wait()
    for q in range(4):
        loads[6 + q].wait()
        OB[q] = lax.dot_general(H[q], DY[...], TN_DIMS, preferred_element_type=F32)
        put(OB.at[q], dwo.at[pl.ds(q * fq, fq)])
    for cp in outs:
        cp.wait()


def solution(mesh):
    act_spec = P(("dp", "row"), "col")
    weight_spec = P("row", "col")

    def block_backward(x_blk, gy_blk, gate_blk, up_blk, out_blk):
        rows, dm = x_blk.shape
        ff = gate_blk.shape[1]
        fq, tok = ff // 4, 4 * rows
        vm = pltpu.VMEM
        xg, dyg, dbg, hg, dxg = pl.pallas_call(
            lambda *refs: comm_kernel(rows, dm, ff, *refs),
            out_shape=[
                jax.ShapeDtypeStruct((dm, tok), BF16),
                jax.ShapeDtypeStruct((2, 2, rows, dm), BF16),
                jax.ShapeDtypeStruct((4, 4, rows, 2 * fq), BF16),
                jax.ShapeDtypeStruct((2, 2, 4, rows, fq), BF16),
                jax.ShapeDtypeStruct((rows, dm), BF16),
            ],
            in_specs=[ANY] * 5,
            out_specs=[ANY] * 5,
            scratch_shapes=[
                vm((2, 2, 2, rows, dm), BF16),
                vm((2, rows, dm), BF16),
                vm((4, 2, 2, rows, dm), BF16),
                vm((4, dm, 2 * fq), BF16),
                vm((2, dm, 2 * fq), BF16),
                vm((fq, 4 * dm), BF16),
                vm((2, fq, dm // 2), BF16),
                vm((4, rows, 2 * fq), F32),
                vm((4, rows, 2 * fq), F32),
                vm((4, max(RBS), 2 * fq), F32),
                vm((4, rows, fq), F32),
                vm((4, 4, rows, 2 * fq), BF16),
                vm((3, 2, 4, rows, fq), BF16),
                vm((2, 4, rows, fq), BF16),
                vm((2, 2, rows, dm), F32),
                vm((2, 2, rows, dm), F32),
                vm((2, 2, rows, dm), F32),
                vm((2, 2, rows, dm), BF16),
                vm((rows, dm), BF16),
                vm((dm, tok), BF16),
                pltpu.SemaphoreType.DMA((N_SEND,)),
                pltpu.SemaphoreType.DMA((N_RECV,)),
                pltpu.SemaphoreType.DMA((N_LOCAL,)),
            ],
            compiler_params=pltpu.CompilerParams(collective_id=0, has_side_effects=True, vmem_limit_bytes=63 * 1024 * 1024),
            name="comm",
        )(x_blk, gy_blk, gate_blk, up_blk, out_blk)
        dw_gate, dw_up, dw_out, grad_x = pl.pallas_call(
            dw_kernel,
            out_shape=[
                jax.ShapeDtypeStruct((dm, ff), F32),
                jax.ShapeDtypeStruct((dm, ff), F32),
                jax.ShapeDtypeStruct((ff, dm), F32),
                jax.ShapeDtypeStruct((rows, dm), BF16),
            ],
            in_specs=[ANY] * 5,
            out_specs=[ANY] * 4,
            scratch_shapes=[
                vm((dm, tok), BF16), vm((tok, dm), BF16),
                vm((4, tok, 2 * fq), BF16), vm((4, tok, fq), BF16), vm((rows, dm), BF16),
                vm((4, dm, 2 * fq), F32), vm((4, fq, dm), F32),
                pltpu.SemaphoreType.DMA((11,)), pltpu.SemaphoreType.DMA((13,)),
            ],
            compiler_params=pltpu.CompilerParams(vmem_limit_bytes=60 * 1024 * 1024),
            name="dw",
        )(xg, dyg.reshape(tok, dm), dbg.reshape(4, tok, 2 * fq), hg.reshape(4, tok, fq), dxg)
        return grad_x, dw_gate, dw_up, dw_out

    return jax.shard_map(block_backward, mesh=mesh, in_specs=(act_spec, act_spec, weight_spec, weight_spec, weight_spec), out_specs=(act_spec, act_spec, act_spec, act_spec), check_vma=False)
```
